32 devices in a mesh: row: 4 (over y, x), col: 8 (over z, core).
Axes of the slice: x: 2, y: 2, z: 4, core: 2. Of those that a mesh axis runs over, the one named last changes fastest.
Arguments:
- coeffs: bfloat16 [16384, 2048], P('row'), may hold values from -1 to 1
- p_slots: int32 [4, 8, 64], P('row', 'col'), may hold values from 0 to 511, as said below
- p_count: int32 [4, 8], P('row', 'col'), may hold values from 1 to 64
- s_blocks: bfloat16 [4, 8, 64, 128, 128], P('row', 'col'), may hold values from -0.3984375 to 0.3984375
- s_slots: int32 [4, 8, 64], P('row', 'col'), may hold values from 0 to 511, as said below
- s_count: int32 [4, 8], P('row', 'col'), may hold values from 1 to 64
- q_slots: int32 [4, 8, 64], P('row', 'col'), may hold values from 0 to 511, as said below
- q_count: int32 [4, 8], P('row', 'col'), may hold values from 1 to 64
Outputs:
- density: bfloat16 [4, 8, 64, 128, 128], P('row', 'col')
- product: float32 [4, 8, 64, 128, 128], P('row', 'col')
The draws below stay inside these ranges and needn't reach their ends.
Inputs may be any that keep to these rules, and one draw needn't show every extreme that they name: `p_slots`: on each device the live slots name different blocks of its tile; at least one device has all 64 slots live, which one is drawn. `s_slots`: on each device the live slots name different positions; at least one device has all 64 slots live, which one is drawn. `q_slots`: on each device the live slots name different blocks of its tile; at least one device has all 64 slots live, which one is drawn.
All inputs are finite; a program needn't handle non-finite values.
Results may differ from the reference program's by a relative error of at most 0.0029.
Values may be sent and summed in bfloat16 or wider, within the bound.
A program may use at most 192 MiB of HBM per device.

```python
import jax
import jax.numpy as jnp
from jax import lax

N = 16384
K = 2048
ROWB = 32
COLB = 16
SPAN = 2
PMAX = 64
QMAX = 64
SMAX = 64
N_ROW = 4
N_COL = 8


def pattern_slots(key, total, most):
    keys = jax.random.split(key, N_ROW * N_COL)
    picks = jax.vmap(lambda single: jax.random.permutation(single, total)[:most])(keys)
    return picks.reshape(N_ROW, N_COL, most).astype(jnp.int32)


def pattern_count(key, most):
    first_key, second_key = jax.random.split(key)
    counts = jax.random.randint(first_key, (N_ROW * N_COL,), 1, most + 1)
    chosen = jax.random.randint(second_key, (), 0, N_ROW * N_COL)
    counts = jnp.where(jnp.arange(N_ROW * N_COL) == chosen, most, counts)
    return counts.reshape(N_ROW, N_COL).astype(jnp.int32)


def draw_p_slots(key, part):
    return pattern_slots(jax.random.fold_in(key, 11), ROWB * COLB, PMAX)


def draw_p_count(key, part):
    return pattern_count(jax.random.fold_in(key, 12), PMAX)


def draw_s_slots(key, part):
    return pattern_slots(jax.random.fold_in(key, 21), SPAN * COLB * COLB, SMAX)


def draw_s_count(key, part):
    return pattern_count(jax.random.fold_in(key, 22), SMAX)


def draw_q_slots(key, part):
    return pattern_slots(jax.random.fold_in(key, 31), ROWB * COLB, QMAX)


def draw_q_count(key, part):
    return pattern_count(jax.random.fold_in(key, 32), QMAX)


def level_of(stream_key, shape, cuts, low, largest):
    def one(dim, blocks):
        steps = jax.random.uniform(jax.random.fold_in(jax.random.fold_in(stream_key, 6), dim), (blocks,), jnp.float32, low / len(cuts), largest / len(cuts))
        return jnp.repeat(jnp.exp(steps), shape[dim] // blocks).reshape((-1,) + (1,) * (len(shape) - dim - 1))

    gain = one(*cuts[0])
    for cut in cuts[1:]:
        gain = gain * one(*cut)
    return gain


def gaussian(own_key, extent, deviation, limit, shards=(), kind=jnp.bfloat16):
    array = jax.random.normal(own_key, extent, jnp.float32) * deviation
    if len(shards) > 0:
        array = level_of(own_key, extent, shards, -0.22, 0.18) * array
    return jnp.clip(array, min=-limit, max=limit).astype(kind)


def setup_inputs(seed: int = 0) -> dict:
    key_list = jax.random.split(jax.random.key(seed), 9)
    return {
        "coeffs": gaussian(key_list[0], (N, K), 0.15, 1.0, ((0, 4),)),
        "p_slots": draw_p_slots(jax.random.fold_in(key_list[8], 71), 0),
        "p_count": draw_p_count(jax.random.fold_in(key_list[8], 71), 0),
        "s_blocks": gaussian(key_list[3], (N_ROW, N_COL, SMAX, 128, 128), 0.0625, 0.3984375, ((0, 4), (1, 8))),
        "s_slots": draw_s_slots(jax.random.fold_in(key_list[8], 71), 0),
        "s_count": draw_s_count(jax.random.fold_in(key_list[8], 71), 0),
        "q_slots": draw_q_slots(jax.random.fold_in(key_list[8], 71), 0),
        "q_count": draw_q_count(jax.random.fold_in(key_list[8], 71), 0),
    }


def reference(coeffs, p_slots, p_count, s_blocks, s_slots, s_count, q_slots, q_count):
    block_count = coeffs.shape[0] // 128
    orbitals = coeffs.shape[1]
    tile_rows = block_count // N_ROW
    tile_cols = block_count // N_COL
    grid_row = jnp.arange(N_ROW, dtype=jnp.int32)[:, None, None]
    grid_col = jnp.arange(N_COL, dtype=jnp.int32)[None, :, None]
    blocked = coeffs.reshape(block_count, 128, orbitals)

    p_live = jnp.arange(p_slots.shape[2], dtype=jnp.int32)[None, None, :] < p_count[:, :, None]
    p_global_row = (grid_row * tile_rows + p_slots // tile_cols).astype(jnp.int32).reshape(-1)
    p_global_col = (grid_col * tile_cols + p_slots % tile_cols).astype(jnp.int32).reshape(-1)

    def density_block(pair):
        return jnp.dot(blocked[pair[0]], blocked[pair[1]].T, preferred_element_type=jnp.float32)

    raw = lax.map(density_block, (p_global_row, p_global_col))
    raw = raw.reshape(N_ROW, N_COL, -1, 128, 128)
    density = jnp.where(p_live[..., None, None], raw, jnp.zeros_like(raw)).astype(jnp.bfloat16)

    dense_p = jnp.zeros((block_count, block_count, 128, 128), jnp.bfloat16)
    dense_p = dense_p.at[p_global_row, p_global_col].add(density.reshape(-1, 128, 128))

    s_live = jnp.arange(s_slots.shape[2], dtype=jnp.int32)[None, None, :] < s_count[:, :, None]
    local_row = s_slots // tile_cols
    panel_index = grid_row + N_ROW * (local_row // tile_cols)
    s_global_row = (panel_index * tile_cols + local_row % tile_cols).astype(jnp.int32).reshape(-1)
    s_global_col = (grid_col * tile_cols + s_slots % tile_cols).astype(jnp.int32).reshape(-1)
    s_kept = jnp.where(s_live[..., None, None], s_blocks, jnp.zeros_like(s_blocks)).reshape(-1, 128, 128)
    dense_s = jnp.zeros((block_count, block_count, 128, 128), jnp.bfloat16)
    dense_s = dense_s.at[s_global_row, s_global_col].add(s_kept)

    q_live = jnp.arange(q_slots.shape[2], dtype=jnp.int32)[None, None, :] < q_count[:, :, None]
    q_global_row = (grid_row * tile_rows + q_slots // tile_cols).astype(jnp.int32).reshape(-1)
    q_global_col = (grid_col * tile_cols + q_slots % tile_cols).astype(jnp.int32).reshape(-1)

    def product_block(pair):
        left = dense_p[pair[0]].astype(jnp.float32)
        right = dense_s[:, pair[1]].astype(jnp.float32)
        return jnp.einsum('kab,kbc->ac', left, right)

    summed = lax.map(product_block, (q_global_row, q_global_col))
    summed = summed.reshape(N_ROW, N_COL, -1, 128, 128)
    product = jnp.where(q_live[..., None, None], summed, jnp.zeros_like(summed))
    return density, product
```

```python
import functools

import jax
import jax.numpy as jnp
from jax import lax
from jax.experimental import pallas as pl
from jax.experimental.pallas import tpu as pltpu
from jax.sharding import PartitionSpec as P

MESH = pl.DeviceIdType.MESH
MIB = 1 << 20
CHUNK = 256
PIECE = 2
DEPTH = 3


def rows_kernel(rows_n, cols_n, coeffs, out, send, recv):
    row, col = lax.axis_index("row"), lax.axis_index("col")
    sub = cols_n // rows_n
    height = out.shape[0]
    piece = height // rows_n
    half, share = lax.rem(col, sub), lax.div(col, sub)
    owner = lax.div(col, sub)
    targets = [
        {"row": lax.rem(row + step, rows_n), "col": row * sub + half} for step in range(1, rows_n)
    ]
    sources = [{"row": owner, "col": part * sub + half} for part in range(rows_n)]
    barrier = pltpu.get_barrier_semaphore()
    for device in targets:
        pl.semaphore_signal(barrier, inc=1, device_id=device, device_id_type=MESH)

    @pl.when(row != owner)
    def _():
        for device in sources:
            pl.semaphore_signal(barrier, inc=1, device_id=device, device_id_type=MESH)

    pl.semaphore_wait(barrier, rows_n - 1 + jnp.where(row != owner, rows_n, 0))

    def copy(step, part, device):
        start = half * height + share * piece
        return pltpu.make_async_remote_copy(
            src_ref=coeffs.at[pl.ds(pl.multiple_of(start, piece), piece)],
            dst_ref=out.at[pl.ds(pl.multiple_of(part * piece, piece), piece)],
            send_sem=send.at[step],
            recv_sem=recv.at[part],
            device_id=device,
            device_id_type=MESH,
        )

    sends = [copy(step, share, device) for step, device in enumerate(targets)]
    for one in sends:
        one.start()

    @pl.when(row != owner)
    def _():
        for part, device in enumerate(sources):
            copy(0, part, device).wait_recv()

    for one in sends:
        one.wait_send()


def gather_rows(coeffs, rows_n, cols_n):
    height = coeffs.shape[0] * rows_n // cols_n
    body = functools.partial(rows_kernel, rows_n, cols_n)
    sems = [pltpu.SemaphoreType.DMA((rows_n - 1,)), pltpu.SemaphoreType.DMA((rows_n,))]
    return pl.pallas_call(
        body,
        out_shape=jax.ShapeDtypeStruct((height, coeffs.shape[1]), coeffs.dtype),
        in_specs=[pl.BlockSpec(memory_space=pl.ANY)],
        out_specs=pl.BlockSpec(memory_space=pl.ANY),
        scratch_shapes=sems,
        compiler_params=pltpu.CompilerParams(collective_id=0, has_side_effects=True),
    )(coeffs)


def density_kernel(rows_n, cols_n, ids, count, coeffs, others, out, left, right, sem):
    row, col = lax.axis_index("row"), lax.axis_index("col")
    sub = cols_n // rows_n
    height = others.shape[0]
    tile_cols = height // 128
    load_left = pltpu.make_async_copy(coeffs, left, sem.at[0])
    load_left.start()
    here = row == lax.div(col, sub)
    start = pl.multiple_of(lax.rem(col, sub) * height, height)
    load_own = pltpu.make_async_copy(coeffs.at[pl.ds(start, height)], right, sem.at[1])
    load_other = pltpu.make_async_copy(others, right, sem.at[1])

    @pl.when(here)
    def _():
        load_own.start()

    @pl.when(jnp.logical_not(here))
    def _():
        load_other.start()

    live = count[0]
    load_left.wait()
    load_other.wait()

    def block(slot, carry):
        a = pl.multiple_of(lax.div(ids[slot], tile_cols) * 128, 128)
        b = pl.multiple_of(lax.rem(ids[slot], tile_cols) * 128, 128)
        raw = lax.dot_general(
            left[pl.ds(a, 128), :],
            right[pl.ds(b, 128), :],
            (((1,), (1,)), ((), ())),
            preferred_element_type=jnp.float32,
        )
        out[slot] = raw.astype(out.dtype)
        return carry

    def clear(slot, carry):
        out[slot] = jnp.zeros(out.shape[1:], out.dtype)
        return carry

    lax.fori_loop(0, live, block, 0)
    lax.fori_loop(live, out.shape[0], clear, 0)


def density(ids, count, coeffs, others, rows_n, cols_n):
    slots = ids.shape[0]
    return pl.pallas_call(
        functools.partial(density_kernel, rows_n, cols_n),
        out_shape=jax.ShapeDtypeStruct((slots, 128, 128), jnp.bfloat16),
        in_specs=[pl.BlockSpec(memory_space=pltpu.SMEM)] * 2
        + [pl.BlockSpec(memory_space=pl.ANY)] * 2,
        out_specs=pl.BlockSpec(memory_space=pltpu.VMEM),
        scratch_shapes=[
            pltpu.VMEM(coeffs.shape, coeffs.dtype),
            pltpu.VMEM(others.shape, coeffs.dtype),
            pltpu.SemaphoreType.DMA((2,)),
        ],
        compiler_params=pltpu.CompilerParams(vmem_limit_bytes=40 * MIB),
    )(ids, count, coeffs, others)


def panel_kernel(rows_n, cols_n, chunks, parts, depth, ids, count, coeffs, out, *scratch):
    left, total, send, recv, sem = scratch[chunks:]
    right = scratch[:chunks]
    row, col = lax.axis_index("row"), lax.axis_index("col")
    sub = cols_n // rows_n
    tile_cols, _, wide = right[0].shape
    size = tile_cols // (2 * parts)
    owner = lax.div(col, sub)
    first = lax.rem(col, sub) * tile_cols
    y, x = lax.div(row, 2), lax.rem(row, 2)
    dy = lax.rem(y + lax.div(owner, 2), 2)
    dx = lax.rem(x + lax.rem(owner, 2), 2)
    along_x, along_y = y * 2 + 1 - x, (1 - y) * 2 + x
    is_source = row == owner
    sends = [jnp.logical_or(dx == 1, dy == 0), jnp.logical_or(dx == 0, dy == 1)]
    following = [
        jnp.where(dx == dy, along_x, along_y),
        jnp.where(dx == dy, along_y, along_x),
    ]
    steps = [(k, part) for k in range(chunks) for part in range(parts)]

    def offset(way, part):
        return (way * parts + part) * size

    def load(way, k, part):
        return pltpu.make_async_copy(
            coeffs.at[pl.ds(first + offset(way, part), size), :, pl.ds(k * wide, wide)],
            right[k].at[pl.ds(offset(way, part), size)],
            recv.at[way, k * parts + part],
        )

    def copy(way, k, part):
        where = right[k].at[pl.ds(offset(way, part), size)]
        return pltpu.make_async_remote_copy(
            src_ref=where,
            dst_ref=where,
            send_sem=send.at[way, k * parts + part],
            recv_sem=recv.at[way, k * parts + part],
            device_id={"row": following[way], "col": col},
            device_id_type=MESH,
        )

    @pl.when(is_source)
    def _():
        for k, part in steps:
            for way in range(2):
                load(way, k, part).start()

    load_left = pltpu.make_async_copy(coeffs, left, sem.at[0])
    load_left.start()
    barrier = pltpu.get_barrier_semaphore()
    for near in (along_x, along_y):
        pl.semaphore_signal(
            barrier, inc=1, device_id={"row": near, "col": col}, device_id_type=MESH
        )
    pl.semaphore_wait(barrier, 2)
    live = count[0]

    def relay(k):
        for part in range(parts):
            now = k * parts + part
            for way in range(2):

                @pl.when(sends[way])
                def _():
                    copy(way, k, part).wait_recv()
                    if now >= depth:
                        copy(way, *steps[now - depth]).wait_send()
                    copy(way, k, part).start()

    relay(0)
    load_left.wait()
    for k in range(chunks):
        if k < chunks - 1:
            relay(k + 1)
        for way in range(2):

            @pl.when(jnp.logical_not(sends[way]))
            def _():
                for part in range(parts):
                    copy(way, k, part).wait_recv()

        def block(slot, carry, k=k):
            raw = lax.dot_general(
                left[lax.div(ids[slot], tile_cols), :, pl.ds(k * wide, wide)],
                right[k][lax.rem(ids[slot], tile_cols)],
                (((1,), (1,)), ((), ())),
                preferred_element_type=jnp.float32,
            )
            if k > 0:
                raw = raw + total[slot]
            if k < chunks - 1:
                total[slot] = raw
            else:
                out[slot] = jnp.where(slot < live, raw, 0.0).astype(out.dtype)
            return carry

        lax.fori_loop(0, out.shape[0], block, 0, unroll=4)

    for way in range(2):

        @pl.when(sends[way])
        def _():
            for k, part in steps[-depth:]:
                copy(way, k, part).wait_send()


def panel_density(ids, count, coeffs, rows_n, cols_n):
    slots = ids.shape[0]
    orbitals = coeffs.shape[1]
    blocks = coeffs.reshape(-1, 128, orbitals)
    tile_cols = blocks.shape[0] * rows_n // cols_n
    chunks = max(1, orbitals // CHUNK)
    parts = max(1, tile_cols // (2 * PIECE))
    return pl.pallas_call(
        functools.partial(panel_kernel, rows_n, cols_n, chunks, parts, DEPTH),
        out_shape=jax.ShapeDtypeStruct((slots, 128, 128), jnp.bfloat16),
        in_specs=[pl.BlockSpec(memory_space=pltpu.SMEM)] * 2
        + [pl.BlockSpec(memory_space=pl.ANY)],
        out_specs=pl.BlockSpec(memory_space=pltpu.VMEM),
        scratch_shapes=[pltpu.VMEM((tile_cols, 128, orbitals // chunks), coeffs.dtype)] * chunks
        + [
            pltpu.VMEM(blocks.shape, coeffs.dtype),
            pltpu.VMEM((slots, 128, 128), jnp.float32),
            pltpu.SemaphoreType.DMA((2, chunks * parts)),
            pltpu.SemaphoreType.DMA((2, chunks * parts)),
            pltpu.SemaphoreType.DMA((1,)),
        ],
        compiler_params=pltpu.CompilerParams(
            collective_id=2, has_side_effects=True, vmem_limit_bytes=40 * MIB
        ),
    )(ids, count, blocks)


def blocks_kernel(rows_n, cols_n, parts, p_own, s_own, p_all, s_all, *sems):
    send, recv, pass_send, pass_recv, s_send, s_recv = sems
    row, col = lax.axis_index("row"), lax.axis_index("col")
    length = cols_n // 2
    z, core = lax.div(col, 2), lax.rem(col, 2)
    size = p_own.shape[0] // parts
    right, left = {"row": row, "col": col + 2}, {"row": row, "col": col - 2}
    partner = {"row": row, "col": z * 2 + 1 - core}
    column = [{"row": lax.rem(row + step, rows_n), "col": col} for step in range(1, rows_n)]
    has_right, has_left = z + 1 < length, z > 0

    barrier = pltpu.get_barrier_semaphore()

    def greet(device):
        pl.semaphore_signal(barrier, inc=1, device_id=device, device_id_type=MESH)

    greet(partner)
    for device in column:
        greet(device)

    @pl.when(has_right)
    def _():
        greet(right)

    @pl.when(has_left)
    def _():
        greet(left)

    pl.semaphore_wait(barrier, rows_n + jnp.where(has_right, 1, 0) + jnp.where(has_left, 1, 0))

    def remote(src, dst, send_sem, recv_sem, device):
        return pltpu.make_async_remote_copy(
            src_ref=src,
            dst_ref=dst,
            send_sem=send_sem,
            recv_sem=recv_sem,
            device_id=device,
            device_id_type=MESH,
        )

    def piece(source, lane, part):
        return p_all.at[source * 2 + lane, pl.ds(part * size, size)]

    def origin(way, step):
        return z - step if way == 0 else z + step

    def sent(way, step, part):
        where = piece(origin(way, step), core, part)
        src = p_own.at[pl.ds(part * size, size)] if step == 0 else where
        device = right if way == 0 else left
        return remote(src, where, send.at[way, step, part], recv.at[way, step, part], device)

    def passed(way, step, part):
        where = piece(origin(way, step), core, part)
        src = p_own.at[pl.ds(part * size, size)] if step == 0 else where
        return remote(
            src, where, pass_send.at[way, step, part], pass_recv.at[way, step, part], partner
        )

    def onward(way):
        return has_right if way == 0 else has_left

    def exists(way, step):
        return z >= step if way == 0 else z + step < length

    for part in range(parts):
        for way in range(2):
            pl.when(onward(way))(lambda way=way: sent(way, 0, part).start())
    s_sends = [
        remote(s_own, s_all.at[row], s_send.at[n], s_recv.at[n], device)
        for n, device in enumerate(column)
    ]
    for one in s_sends:
        one.start()
    for part in range(parts):
        passed(0, 0, part).start()
    for step in range(1, length):
        for part in range(parts):
            for way in range(2):

                @pl.when(exists(way, step))
                def _():
                    sent(way, step - 1, part).wait_recv()
                    passed(way, step, part).start()
                    if step < length - 1:
                        pl.when(onward(way))(lambda: sent(way, step, part).start())

    for part in range(parts):
        passed(0, 0, part).wait()
        for way in range(2):
            pl.when(onward(way))(lambda way=way: sent(way, 0, part).wait_send())
    for step in range(1, length):
        for part in range(parts):
            for way in range(2):

                @pl.when(exists(way, step))
                def _():
                    passed(way, step, part).wait()
                    if step < length - 1:
                        pl.when(onward(way))(lambda: sent(way, step, part).wait_send())

    for one in s_sends:
        one.wait()


def gather_blocks(p_own, s_own, rows_n, cols_n):
    parts = 4 if p_own.shape[0] % 4 == 0 else 1
    table = pltpu.SemaphoreType.DMA((2, cols_n // 2, parts))
    return pl.pallas_call(
        functools.partial(blocks_kernel, rows_n, cols_n, parts),
        out_shape=(
            jax.ShapeDtypeStruct((cols_n,) + p_own.shape, p_own.dtype),
            jax.ShapeDtypeStruct((rows_n,) + s_own.shape, s_own.dtype),
        ),
        in_specs=[pl.BlockSpec(memory_space=pl.ANY)] * 2,
        out_specs=[pl.BlockSpec(memory_space=pl.ANY)] * 2,
        scratch_shapes=[table] * 4 + [pltpu.SemaphoreType.DMA((rows_n - 1,))] * 2,
        compiler_params=pltpu.CompilerParams(collective_id=1, has_side_effects=True),
    )(p_own, s_own)


def product_kernel(rows_n, cols_n, codes, counts, p_own, s_own, p_all, s_all, out, left, right, sem):
    row, col = lax.axis_index("row"), lax.axis_index("col")
    p_max, s_max = p_own.shape[0], s_own.shape[0]
    base = rows_n * s_max
    loads = [pltpu.make_async_copy(p_own, left.at[pl.ds(col * p_max, p_max)], sem.at[0])]
    loads += [pltpu.make_async_copy(s_own, right.at[pl.ds(row * s_max, s_max)], sem.at[1])]
    for step in range(1, cols_n):
        at = lax.rem(col + step, cols_n)
        loads += [
            pltpu.make_async_copy(
                p_all.at[at], left.at[pl.ds(at * p_max, p_max)], sem.at[len(loads)]
            )
        ]
    for step in range(1, rows_n):
        at = lax.rem(row + step, rows_n)
        loads += [
            pltpu.make_async_copy(
                s_all.at[at], right.at[pl.ds(at * s_max, s_max)], sem.at[len(loads)]
            )
        ]
    for load in loads:
        load.start()
    for load in loads:
        load.wait()

    def slot(q, carry):
        def term(n, total):
            code = codes[q, n]
            return total + jnp.dot(
                left[lax.div(code, base)],
                right[lax.rem(code, base)],
                preferred_element_type=jnp.float32,
            )

        out[q] = lax.fori_loop(0, counts[q], term, jnp.zeros((128, 128), jnp.float32))
        return carry

    lax.fori_loop(0, out.shape[0], slot, 0)


def block_product(codes, counts, p_own, s_own, p_all, s_all):
    cols_n, p_max = p_all.shape[:2]
    rows_n, s_max = s_all.shape[:2]
    return pl.pallas_call(
        functools.partial(product_kernel, rows_n, cols_n),
        out_shape=jax.ShapeDtypeStruct((counts.shape[0], 128, 128), jnp.float32),
        in_specs=[pl.BlockSpec(memory_space=pltpu.SMEM)] * 2
        + [pl.BlockSpec(memory_space=pl.ANY)] * 4,
        out_specs=pl.BlockSpec(memory_space=pltpu.VMEM),
        scratch_shapes=[
            pltpu.VMEM((cols_n * p_max, 128, 128), p_all.dtype),
            pltpu.VMEM((rows_n * s_max, 128, 128), s_all.dtype),
            pltpu.SemaphoreType.DMA((cols_n + rows_n,)),
        ],
        compiler_params=pltpu.CompilerParams(vmem_limit_bytes=40 * MIB),
    )(codes, counts, p_own, s_own, p_all, s_all)


def match_lists(p_codes, s_codes, q_ids, q_live, tile_cols, span):
    cols_n, p_max = p_codes.shape
    rows_n, s_max = s_codes.shape
    q_row, q_col = q_ids // tile_cols, q_ids % tile_cols
    at = jnp.arange(tile_cols, dtype=jnp.int32)
    p_want = q_row[:, None] * tile_cols + at[None, :]
    p_hit = p_codes[None, :, None, :] == p_want[:, None, :, None]
    p_slot = jnp.arange(cols_n * p_max, dtype=jnp.int32).reshape(1, cols_n, 1, p_max)
    p_at = jnp.max(jnp.where(p_hit, p_slot, -1), axis=3)
    level = jnp.arange(span * tile_cols, dtype=jnp.int32).reshape(span, tile_cols)
    s_want = level[None] * tile_cols + q_col[:, None, None]
    s_hit = s_codes[None, None, :, None, :] == s_want[:, :, None, :, None]
    s_slot = jnp.arange(rows_n * s_max, dtype=jnp.int32).reshape(1, 1, rows_n, 1, s_max)
    s_at = jnp.max(jnp.where(s_hit, s_slot, -1), axis=4)
    p_at = p_at.reshape(q_ids.shape[0], -1)
    s_at = s_at.reshape(q_ids.shape[0], -1)
    depth = p_at.shape[1]
    match = (p_at >= 0) & (s_at >= 0) & q_live[:, None]
    code = jnp.where(match, p_at * (rows_n * s_max) + s_at, 0)
    order = jnp.arange(depth, dtype=jnp.int32)
    before = order[None, :, None] > order[None, None, :]
    rank = jnp.sum((before & match[:, None, :]).astype(jnp.int32), axis=2)
    rank = jnp.where(match, rank, -1)
    picked = rank[:, None, :] == order[None, :, None]
    codes = jnp.sum(jnp.where(picked, code[:, None, :], 0), axis=2)
    return codes, jnp.sum(match.astype(jnp.int32), axis=1)


def on_device(coeffs, p_slots, p_count, s_blocks, s_slots, s_count, q_slots, q_count):
    rows_n = lax.axis_size("row")
    cols_n = lax.axis_size("col")
    tile_cols = coeffs.shape[0] * rows_n // cols_n // 128
    p_ids, s_ids, q_ids = p_slots[0, 0], s_slots[0, 0], q_slots[0, 0]
    s_own = s_blocks[0, 0]
    p_max, s_max, q_max = p_ids.shape[0], s_ids.shape[0], q_ids.shape[0]

    def live(ids, count):
        return jnp.arange(ids.shape[0], dtype=jnp.int32) < count[0, 0]

    p_codes = lax.all_gather(jnp.where(live(p_ids, p_count), p_ids, -1), "col")
    s_codes = lax.all_gather(jnp.where(live(s_ids, s_count), s_ids, -1), "row")
    codes, counts = match_lists(
        p_codes, s_codes, q_ids, live(q_ids, q_count), tile_cols, cols_n // rows_n
    )
    if rows_n == 4:
        p_own = panel_density(p_ids, p_count[0], coeffs, rows_n, cols_n)
    else:
        others = gather_rows(coeffs, rows_n, cols_n)
        p_own = density(p_ids, p_count[0], coeffs, others, rows_n, cols_n)
    p_all, s_all = gather_blocks(p_own, s_own, rows_n, cols_n)
    product = block_product(codes, counts, p_own, s_own, p_all, s_all)
    return (p_own.reshape(1, 1, p_max, 128, 128), product.reshape(1, 1, q_max, 128, 128))


def solution(mesh):
    return jax.shard_map(
        on_device,
        mesh=mesh,
        in_specs=(
            P("row", None),
            P("row", "col", None),
            P("row", "col"),
            P("row", "col", None, None, None),
            P("row", "col", None),
            P("row", "col"),
            P("row", "col", None),
            P("row", "col"),
        ),
        out_specs=(P("row", "col", None, None, None), P("row", "col", None, None, None)),
        check_vma=False,
    )
```

```python
import functools

import jax
import jax.numpy as jnp
from jax import lax
from jax.experimental import pallas as pl
from jax.experimental.pallas import tpu as pltpu
from jax.sharding import PartitionSpec as P

MESH = pl.DeviceIdType.MESH
MIB = 1 << 20
CHUNK = 256
PIECE = 2
DEPTH = 3
LANES = 128
CODE = 512
P_CAP = 44
S_CAP = 32


def rows_kernel(rows_n, cols_n, coeffs, out, send, recv):
    row, col = lax.axis_index("row"), lax.axis_index("col")
    sub = cols_n // rows_n
    height = out.shape[0]
    piece = height // rows_n
    half, share = lax.rem(col, sub), lax.div(col, sub)
    owner = lax.div(col, sub)
    targets = [
        {"row": lax.rem(row + step, rows_n), "col": row * sub + half} for step in range(1, rows_n)
    ]
    sources = [{"row": owner, "col": part * sub + half} for part in range(rows_n)]
    barrier = pltpu.get_barrier_semaphore()
    for device in targets:
        pl.semaphore_signal(barrier, inc=1, device_id=device, device_id_type=MESH)

    @pl.when(row != owner)
    def _():
        for device in sources:
            pl.semaphore_signal(barrier, inc=1, device_id=device, device_id_type=MESH)

    pl.semaphore_wait(barrier, rows_n - 1 + jnp.where(row != owner, rows_n, 0))

    def copy(step, part, device):
        start = half * height + share * piece
        return pltpu.make_async_remote_copy(
            src_ref=coeffs.at[pl.ds(pl.multiple_of(start, piece), piece)],
            dst_ref=out.at[pl.ds(pl.multiple_of(part * piece, piece), piece)],
            send_sem=send.at[step],
            recv_sem=recv.at[part],
            device_id=device,
            device_id_type=MESH,
        )

    sends = [copy(step, share, device) for step, device in enumerate(targets)]
    for one in sends:
        one.start()

    @pl.when(row != owner)
    def _():
        for part, device in enumerate(sources):
            copy(0, part, device).wait_recv()

    for one in sends:
        one.wait_send()


def gather_rows(coeffs, rows_n, cols_n):
    height = coeffs.shape[0] * rows_n // cols_n
    body = functools.partial(rows_kernel, rows_n, cols_n)
    sems = [pltpu.SemaphoreType.DMA((rows_n - 1,)), pltpu.SemaphoreType.DMA((rows_n,))]
    return pl.pallas_call(
        body,
        out_shape=jax.ShapeDtypeStruct((height, coeffs.shape[1]), coeffs.dtype),
        in_specs=[pl.BlockSpec(memory_space=pl.ANY)],
        out_specs=pl.BlockSpec(memory_space=pl.ANY),
        scratch_shapes=sems,
        compiler_params=pltpu.CompilerParams(collective_id=0, has_side_effects=True),
    )(coeffs)


def density_kernel(rows_n, cols_n, ids, count, coeffs, others, out, left, right, sem):
    row, col = lax.axis_index("row"), lax.axis_index("col")
    sub = cols_n // rows_n
    height = others.shape[0]
    tile_cols = height // 128
    load_left = pltpu.make_async_copy(coeffs, left, sem.at[0])
    load_left.start()
    here = row == lax.div(col, sub)
    start = pl.multiple_of(lax.rem(col, sub) * height, height)
    load_own = pltpu.make_async_copy(coeffs.at[pl.ds(start, height)], right, sem.at[1])
    load_other = pltpu.make_async_copy(others, right, sem.at[1])

    @pl.when(here)
    def _():
        load_own.start()

    @pl.when(jnp.logical_not(here))
    def _():
        load_other.start()

    live = count[0]
    load_left.wait()
    load_other.wait()

    def block(slot, carry):
        a = pl.multiple_of(lax.div(ids[slot], tile_cols) * 128, 128)
        b = pl.multiple_of(lax.rem(ids[slot], tile_cols) * 128, 128)
        raw = lax.dot_general(
            left[pl.ds(a, 128), :],
            right[pl.ds(b, 128), :],
            (((1,), (1,)), ((), ())),
            preferred_element_type=jnp.float32,
        )
        out[slot] = raw.astype(out.dtype)
        return carry

    def clear(slot, carry):
        out[slot] = jnp.zeros(out.shape[1:], out.dtype)
        return carry

    lax.fori_loop(0, live, block, 0)
    lax.fori_loop(live, out.shape[0], clear, 0)


def density(ids, count, coeffs, others, rows_n, cols_n):
    slots = ids.shape[0]
    return pl.pallas_call(
        functools.partial(density_kernel, rows_n, cols_n),
        out_shape=jax.ShapeDtypeStruct((slots, 128, 128), jnp.bfloat16),
        in_specs=[pl.BlockSpec(memory_space=pltpu.SMEM)] * 2
        + [pl.BlockSpec(memory_space=pl.ANY)] * 2,
        out_specs=pl.BlockSpec(memory_space=pltpu.VMEM),
        scratch_shapes=[
            pltpu.VMEM(coeffs.shape, coeffs.dtype),
            pltpu.VMEM(others.shape, coeffs.dtype),
            pltpu.SemaphoreType.DMA((2,)),
        ],
        compiler_params=pltpu.CompilerParams(vmem_limit_bytes=40 * MIB),
    )(ids, count, coeffs, others)


def nt(x, y, precision=None):
    return lax.dot_general(
        x, y, (((1,), (1,)), ((), ())), precision=precision, preferred_element_type=jnp.float32
    )


def nn(x, y, precision=None):
    return jnp.dot(x, y, precision=precision, preferred_element_type=jnp.float32)


def iota(shape, dim):
    return lax.broadcasted_iota(jnp.int32, shape, dim)


def onehot(codes, height, kind=jnp.bfloat16):
    hit = iota((height, LANES), 0) == codes
    return jnp.where(hit, 1.0, 0.0).astype(kind)


def flat(x):
    return jnp.minimum(x, 1.0).astype(jnp.bfloat16)


def panel_kernel(rows_n, cols_n, chunks, parts, depth, *refs):
    ids, count, p_row, p_live, q_row, q_live, s_row, s_live, coeffs, s_in = refs[:10]
    density, p_pair_out, p_recv, s_recv, codes, counts, flags_out, meta_out = refs[10:18]
    right = refs[18 : 18 + chunks]
    (
        left, total, p_pair, s_own, p_pack, s_pack, meta, flags,
        p_dense, q_dense, q_wide, s_dense, p_need, p_rank, s_need, s_rank, lists, lists_s,
        send, recv, sem, meta_send, meta_recv, flag_send, flag_recv,
        pair_send, pair_recv, p_send, p_got, pass_send, pass_recv, s_send, s_got, done,
    ) = refs[18 + chunks :]
    row, col = lax.axis_index("row"), lax.axis_index("col")
    slots = ids.shape[0]
    sub = cols_n // rows_n
    zs = cols_n // 2
    tile_rows = left.shape[0]
    tile_cols, _, wide = right[0].shape
    bits = tile_cols.bit_length() - 1
    size = tile_cols // (2 * parts)
    p_cap, s_cap = p_recv.shape[1] * p_recv.shape[2], s_recv.shape[1]
    z, core = lax.div(col, 2), lax.rem(col, 2)
    owner = lax.div(col, sub)
    first = lax.rem(col, sub) * tile_cols
    y, x = lax.div(row, 2), lax.rem(row, 2)
    dy = lax.rem(y + lax.div(owner, 2), 2)
    dx = lax.rem(x + lax.rem(owner, 2), 2)
    along_x, along_y = y * 2 + 1 - x, (1 - y) * 2 + x
    is_source = row == owner
    sends = [jnp.logical_or(dx == 1, dy == 0), jnp.logical_or(dx == 0, dy == 1)]
    following = [
        jnp.where(dx == dy, along_x, along_y),
        jnp.where(dx == dy, along_y, along_x),
    ]
    steps = [(k, part) for k in range(chunks) for part in range(parts)]
    partner = {"row": row, "col": z * 2 + 1 - core}
    row_mates = [{"row": row, "col": lax.rem(col + n, cols_n)} for n in range(1, cols_n)]
    col_mates = [{"row": lax.rem(row + n, rows_n), "col": col} for n in range(1, rows_n)]

    def remote(src, dst, send_sem, recv_sem, device):
        return pltpu.make_async_remote_copy(
            src_ref=src,
            dst_ref=dst,
            send_sem=send_sem,
            recv_sem=recv_sem,
            device_id=device,
            device_id_type=MESH,
        )

    def offset(way, part):
        return (way * parts + part) * size

    def load(way, k, part):
        return pltpu.make_async_copy(
            coeffs.at[pl.ds(first + offset(way, part), size), :, pl.ds(k * wide, wide)],
            right[k].at[pl.ds(offset(way, part), size)],
            recv.at[way, k * parts + part],
        )

    def copy(way, k, part):
        where = right[k].at[pl.ds(offset(way, part), size)]
        device = {"row": following[way], "col": col}
        at = k * parts + part
        return remote(where, where, send.at[way, at], recv.at[way, at], device)

    @pl.when(is_source)
    def _():
        for k, part in steps:
            for way in range(2):
                load(way, k, part).start()

    load_left = pltpu.make_async_copy(coeffs, left, sem.at[0])
    load_s = pltpu.make_async_copy(s_in, s_own, sem.at[1])
    load_left.start()
    load_s.start()

    mine = jnp.full((8, LANES), -1, jnp.int32)
    lane = iota((8, LANES), 1)
    height = iota((8, LANES), 0)
    for at, (codes_in, live_in) in enumerate(((p_row, p_live), (q_row, q_live), (s_row, s_live))):
        keep = jnp.logical_and(height == at, lane < live_in[0])
        mine = jnp.where(keep, codes_in[...], mine)
    meta[row, col] = mine

    barrier = pltpu.get_barrier_semaphore()
    for device in row_mates + col_mates:
        pl.semaphore_signal(barrier, inc=1, device_id=device, device_id_type=MESH)
    pl.semaphore_wait(barrier, len(row_mates) + len(col_mates))

    def along_row(table, send_sem, recv_sem, source, n):
        where = table.at[row, source]
        return remote(where, where, send_sem.at[n], recv_sem.at[source], row_mates[n])

    def along_col(table, send_sem, recv_sem, source, n):
        where = table.at[source]
        at = len(row_mates) + n
        return remote(where, where, send_sem.at[at], recv_sem.at[cols_n + source], col_mates[n])

    def spread(table, send_sem, recv_sem):
        def first_half():
            for n in range(cols_n - 1):
                along_row(table, send_sem, recv_sem, col, n).start()

        def second_half():
            for n in range(cols_n - 1):
                source = lax.rem(col + cols_n - 1 - n, cols_n)
                along_row(table, send_sem, recv_sem, source, n).wait_recv()
            for n in range(rows_n - 1):
                along_col(table, send_sem, recv_sem, row, n).start()

        def last():
            for n in range(rows_n - 1):
                source = lax.rem(row + rows_n - 1 - n, rows_n)
                along_col(table, send_sem, recv_sem, source, n).wait_recv()
            for n in range(cols_n - 1):
                along_row(table, send_sem, recv_sem, col, n).wait_send()
            for n in range(rows_n - 1):
                along_col(table, send_sem, recv_sem, row, n).wait_send()

        return first_half, second_half, last

    meta_steps = spread(meta, meta_send, meta_recv)
    flag_steps = spread(flags, flag_send, flag_recv)
    meta_steps[0]()

    def code(at, r, c):
        return meta[r, c][at : at + 1]

    def split(at, r, c):
        value = code(at, r, c)
        return value >> bits, c * tile_cols + (value & (tile_cols - 1))

    def split_s(r, c):
        value = code(2, r, c)
        local = value >> bits
        k = (r + rows_n * (local >> bits)) * tile_cols + (local & (tile_cols - 1))
        return k, c * tile_cols + (value & (tile_cols - 1))

    lanes = iota((1, LANES), 1)
    ahead = jnp.where(iota((LANES, LANES), 0) <= iota((LANES, LANES), 1), 1.0, 0.0)
    ahead = ahead.astype(jnp.bfloat16)
    exact = lax.Precision.HIGHEST

    def dense_rows(r):
        p_sum = jnp.zeros((LANES, tile_rows), jnp.float32)
        q_sum = jnp.zeros((LANES, tile_rows), jnp.float32)
        q_turn = jnp.zeros((tile_rows, LANES), jnp.float32)
        for c in range(cols_n):
            a, k = split(0, r, c)
            p_sum += nt(onehot(k, LANES), onehot(a, tile_rows))
            a, k = split(1, r, c)
            at_row, at_col = onehot(a, tile_rows), onehot(k, LANES)
            q_sum += nt(at_col, at_row)
            q_turn += nt(at_row, at_col)
        p_dense[r] = p_sum.astype(jnp.bfloat16)
        q_dense[r] = q_sum.astype(jnp.bfloat16)
        q_wide[r] = q_turn.astype(jnp.bfloat16)

    def dense_s():
        s_sum = jnp.zeros((LANES, LANES), jnp.float32)
        for r in range(rows_n):
            for c in range(cols_n):
                k, j = split_s(r, c)
                s_sum += nt(onehot(k, LANES), onehot(j, LANES))
        s_dense[...] = s_sum.astype(jnp.bfloat16)

    def need_p():
        wants = []
        for d in range(zs):
            group = lax.broadcasted_iota(jnp.int32, (tile_rows, LANES), 1) // (2 * tile_cols)
            part = jnp.where(group == d, q_wide[row].astype(jnp.float32), 0.0)
            wants.append(flat(nt(s_dense[...], part.astype(jnp.bfloat16))))
        for c in range(cols_n):
            a, k = split(0, row, c)
            at_row, at_k = onehot(a, tile_rows), onehot(k, LANES, jnp.float32)
            for d in range(zs):
                hit = jnp.sum(nn(wants[d], at_row) * at_k, axis=0, keepdims=True)
                p_need[pl.ds(d * cols_n + c, 1)] = jnp.minimum(hit, 1.0)
        rank = nn(p_need[: zs * cols_n].astype(jnp.bfloat16), ahead)
        before = pltpu.roll(jnp.max(rank, axis=1, keepdims=True) + jnp.zeros_like(rank), 1, 0)
        odd = iota(rank.shape, 0) % 2 == 1
        p_rank[: zs * cols_n] = rank + jnp.where(odd, before, 0.0)

    def need_s():
        for r in range(rows_n):
            wants = flat(nt(q_dense[r], p_dense[r]))
            for source in range(rows_n):
                k, j = split_s(source, col)
                hit = nn(wants, onehot(k, LANES)) * onehot(j, LANES, jnp.float32)
                hit = jnp.sum(hit, axis=0, keepdims=True)
                s_need[pl.ds(r * rows_n + source, 1)] = jnp.minimum(hit, 1.0)
        square = rows_n * rows_n
        s_rank[:square] = nn(s_need[:square].astype(jnp.bfloat16), ahead)

    def picks(need, rank, base):
        chosen = jnp.logical_and(rank == (iota((LANES, LANES), 0) + 1).astype(jnp.float32), need > 0)
        chosen = jnp.where(chosen, 1.0, 0.0).astype(jnp.bfloat16)
        values = (base + lane).astype(jnp.float32).astype(jnp.bfloat16)
        return nt(values, chosen)

    def make_lists():
        made = jnp.zeros((8, LANES), jnp.float32)
        for d in range(zs):
            entry = jnp.zeros((8, LANES), jnp.float32)
            for half in range(2):
                at = d * cols_n + z * 2 + half
                entry += picks(p_need[pl.ds(at, 1)], p_rank[pl.ds(at, 1)], half * slots)
            made = jnp.where(height == d, entry, made)
        for r in range(rows_n):
            at = r * rows_n + row
            entry = picks(s_need[pl.ds(at, 1)], s_rank[pl.ds(at, 1)], 0)
            made = jnp.where(height == zs + r, entry, made)
        lists[...] = made.astype(jnp.int32)
        over = jnp.zeros((1, 1), jnp.float32)
        for d in range(zs):
            most = jnp.max(p_rank[pl.ds(z * cols_n + d * 2 + 1, 1)], axis=1, keepdims=True)
            over = jnp.maximum(over, jnp.where(d == z, 0.0, most - p_cap))
        for r in range(rows_n):
            most = jnp.max(s_rank[pl.ds(row * rows_n + r, 1)], axis=1, keepdims=True)
            over = jnp.maximum(over, jnp.where(r == row, 0.0, most - s_cap))
        flags[row, col] = (over + jnp.zeros((8, LANES), jnp.float32)).astype(jnp.int32)

    def make_codes():
        p_at = jnp.zeros((tile_rows, LANES), jnp.float32)
        for c in range(cols_n):
            a, k = split(0, row, c)
            at = z * cols_n + c
            own = (c % 2 * slots + 1 + lanes).astype(jnp.float32)
            far = 2 * slots + c // 2 * p_cap + p_rank[pl.ds(at, 1)]
            far = jnp.where(p_need[pl.ds(at, 1)] > 0, far, 0.0)
            place = jnp.where(c // 2 == z, own, far)
            p_at += nt(
                onehot(a, tile_rows, jnp.float32) * place, onehot(k, LANES, jnp.float32), exact
            )
        s_at = jnp.zeros((LANES, LANES), jnp.float32)
        for r in range(rows_n):
            k, j = split_s(r, col)
            at = row * rows_n + r
            own = (1 + lanes).astype(jnp.float32)
            far = slots + r * s_cap + s_rank[pl.ds(at, 1)]
            far = jnp.where(s_need[pl.ds(at, 1)] > 0, far, 0.0)
            place = jnp.where(r == row, own, far)
            s_at += nt(onehot(j, LANES, jnp.float32) * place, onehot(k, LANES, jnp.float32), exact)
        a, j = split(1, row, col)
        unit = onehot(lanes, LANES)
        q_row_hot = nt(unit, onehot(a, tile_rows))[:slots]
        q_col_hot = nt(unit, onehot(j, LANES))[:slots]
        p_for = nn(q_row_hot, p_at, exact)
        s_for = nn(q_col_hot, s_at, exact)
        match = jnp.where(jnp.logical_and(p_for > 0, s_for > 0), 1.0, 0.0)
        value = (p_for - 1) * CODE + (s_for - 1)
        rank = nn(match.astype(jnp.bfloat16), ahead) * match
        counts[...] = nt(
            jnp.ones((8, LANES), jnp.bfloat16), match.astype(jnp.bfloat16)
        ).astype(jnp.int32)

        def place_one(n, made):
            here = jnp.where(rank == (n + 1).astype(jnp.float32), value, 0.0)
            here = jnp.sum(here, axis=1, keepdims=True)
            return jnp.where(iota(made.shape, 1) == n, here, made)

        made = lax.fori_loop(0, LANES, place_one, jnp.zeros((slots, LANES), jnp.float32))
        codes[...] = made.astype(jnp.int32)

    load_lists = pltpu.make_async_copy(lists, lists_s, sem.at[2])

    def before_three():
        make_lists()
        flag_steps[0]()
        load_lists.start()

    work = {
        0: [meta_steps[1], meta_steps[2]],
        1: [lambda: dense_rows(0), lambda: dense_rows(1)],
        2: [lambda: dense_rows(2), lambda: dense_rows(3), dense_s],
        3: [need_p],
        4: [need_s, before_three],
        5: [flag_steps[1], make_codes],
        6: [flag_steps[2]],
    }

    def relay(k):
        for part in range(parts):
            now = k * parts + part
            for way in range(2):

                @pl.when(sends[way])
                def _():
                    copy(way, k, part).wait_recv()
                    if now >= depth:
                        copy(way, *steps[now - depth]).wait_send()
                    copy(way, k, part).start()

    groups = 4
    group = slots // groups

    def pair_copy(n):
        where = p_pair.at[pl.ds(core * slots + n * group, group)]
        return remote(where, where, pair_send.at[n], pair_recv.at[n], partner)

    def pair_got(n):
        where = p_pair.at[pl.ds((1 - core) * slots + n * group, group)]
        return remote(where, where, pair_send.at[n], pair_recv.at[n], partner)

    relay(0)
    load_left.wait()
    for k in range(chunks):
        if k < chunks - 1:
            relay(k + 1)
        for way in range(2):

            @pl.when(jnp.logical_not(sends[way]))
            def _():
                for part in range(parts):
                    copy(way, k, part).wait_recv()

        def block(slot, carry, k=k):
            raw = lax.dot_general(
                left[ids[slot] >> bits, :, pl.ds(k * wide, wide)],
                right[k][ids[slot] & (tile_cols - 1)],
                (((1,), (1,)), ((), ())),
                preferred_element_type=jnp.float32,
            )
            if k > 0:
                raw = raw + total[slot]
            if k < chunks - 1:
                total[slot] = raw
            else:
                raw = jnp.where(slot < count[0], raw, 0.0)
                p_pair[core * slots + slot] = raw.astype(p_pair.dtype)
            return carry

        if k < chunks - 1:
            lax.fori_loop(0, slots, block, 0, unroll=4)
            for one in work.get(k, []):
                one()
        else:
            for n in range(groups):
                lax.fori_loop(n * group, (n + 1) * group, block, 0, unroll=4)
                pair_copy(n).start()

    density_out = pltpu.make_async_copy(p_pair.at[pl.ds(core * slots, slots)], density, done.at[0])
    density_out.start()
    load_s.wait()
    load_lists.wait()

    def s_copy(n):
        r = col_mates[n]["row"]
        return remote(s_pack.at[n], s_recv.at[row], s_send.at[n], s_got.at[row], col_mates[n])

    def s_arrival(n):
        source = col_mates[n]["row"]
        return remote(s_pack.at[n], s_recv.at[source], s_send.at[n], s_got.at[source], col_mates[n])

    for n in range(groups):
        pair_got(n).wait_recv()
    pair_out = pltpu.make_async_copy(p_pair, p_pair_out, done.at[1])
    pair_out.start()

    def chip(n):
        return lax.rem(z + n + 1, zs)

    def p_copy(n):
        device = {"row": row, "col": chip(n) * 2 + core}
        return remote(p_pack.at[n], p_recv.at[z, core], p_send.at[n], p_got.at[z], device)

    def p_arrival(n):
        where = p_recv.at[chip(n), core]
        return remote(p_pack.at[n], where, p_send.at[n], p_got.at[chip(n)], partner)

    def p_pass(n, half):
        where = p_recv.at[chip(n), half]
        return remote(where, where, pass_send.at[n], pass_recv.at[chip(n)], partner)

    for n in range(zs - 1):
        start = core * (p_cap // 2)

        def fill(t, carry, n=n):
            at = lists_s[chip(n), core * (p_cap // 2) + t]
            p_pack[n, t] = p_pair[jnp.clip(at, 0, 2 * slots - 1)]
            return carry

        lax.fori_loop(0, p_cap // 2, fill, 0, unroll=2)
        p_copy(n).start()
    for n in range(rows_n - 1):

        def fill_s(t, carry, n=n):
            at = lists_s[zs + col_mates[n]["row"], t]
            s_pack[n, t] = s_own[jnp.clip(at, 0, s_own.shape[0] - 1)]
            return carry

        lax.fori_loop(0, s_cap, fill_s, 0, unroll=2)
        s_copy(n).start()

    flags_go = pltpu.make_async_copy(flags, flags_out, done.at[2])
    meta_go = pltpu.make_async_copy(meta, meta_out, done.at[3])
    flags_go.start()
    meta_go.start()
    for way in range(2):

        @pl.when(sends[way])
        def _():
            for k, part in steps[-depth:]:
                copy(way, k, part).wait_send()

    for n in range(groups):
        pair_copy(n).wait_send()
    for n in range(zs - 1):
        p_arrival(n).wait_recv()
        p_pass(n, core).start()
    for n in range(rows_n - 1):
        s_arrival(n).wait_recv()
        s_copy(n).wait_send()
    for n in range(zs - 1):
        p_pass(n, 1 - core).wait_recv()
        p_pass(n, core).wait_send()
        p_copy(n).wait_send()
    density_out.wait()
    pair_out.wait()
    flags_go.wait()
    meta_go.wait()


def panel_density(ids, counts, coeffs, s_own, rows_n, cols_n):
    slots = ids[0].shape[0]
    orbitals = coeffs.shape[1]
    blocks = coeffs.reshape(-1, 128, orbitals)
    tile_rows = blocks.shape[0]
    tile_cols = tile_rows * rows_n // cols_n
    chunks = max(1, orbitals // CHUNK)
    parts = max(1, tile_cols // (2 * PIECE))
    zs = cols_n // 2
    half = P_CAP // 2
    kind = coeffs.dtype
    block = (128, 128)
    smem, vmem = pl.BlockSpec(memory_space=pltpu.SMEM), pl.BlockSpec(memory_space=pltpu.VMEM)
    anywhere = pl.BlockSpec(memory_space=pl.ANY)
    rows = [jnp.pad(one[None], ((0, 0), (0, LANES - slots)), constant_values=-1) for one in ids]
    table = (rows_n, cols_n, 8, LANES)
    sems = pltpu.SemaphoreType.DMA
    floats = [
        pltpu.VMEM((rows_n, LANES, tile_rows), jnp.bfloat16),
        pltpu.VMEM((rows_n, LANES, tile_rows), jnp.bfloat16),
        pltpu.VMEM((rows_n, tile_rows, LANES), jnp.bfloat16),
        pltpu.VMEM((LANES, LANES), jnp.bfloat16),
        pltpu.VMEM((zs * cols_n + 8, LANES), jnp.float32),
        pltpu.VMEM((zs * cols_n + 8, LANES), jnp.float32),
        pltpu.VMEM((rows_n * rows_n + 8, LANES), jnp.float32),
        pltpu.VMEM((rows_n * rows_n + 8, LANES), jnp.float32),
    ]
    return pl.pallas_call(
        functools.partial(panel_kernel, rows_n, cols_n, chunks, parts, DEPTH),
        out_shape=(
            jax.ShapeDtypeStruct((slots,) + block, kind),
            jax.ShapeDtypeStruct((2 * slots,) + block, kind),
            jax.ShapeDtypeStruct((zs, 2, half) + block, kind),
            jax.ShapeDtypeStruct((rows_n, S_CAP) + block, kind),
            jax.ShapeDtypeStruct((slots, LANES), jnp.int32),
            jax.ShapeDtypeStruct((8, slots), jnp.int32),
            jax.ShapeDtypeStruct(table, jnp.int32),
            jax.ShapeDtypeStruct(table, jnp.int32),
        ),
        in_specs=[smem, smem] + [vmem, smem] * 3 + [anywhere] * 2,
        out_specs=[anywhere] * 4 + [vmem] * 2 + [anywhere] * 2,
        scratch_shapes=[pltpu.VMEM((tile_cols, 128, orbitals // chunks), kind)] * chunks
        + [
            pltpu.VMEM(blocks.shape, kind),
            pltpu.VMEM((slots,) + block, jnp.float32),
            pltpu.VMEM((2 * slots,) + block, kind),
            pltpu.VMEM((slots,) + block, kind),
            pltpu.VMEM((zs - 1, half) + block, kind),
            pltpu.VMEM((rows_n - 1, S_CAP) + block, kind),
            pltpu.VMEM(table, jnp.int32),
            pltpu.VMEM(table, jnp.int32),
        ]
        + floats
        + [
            pltpu.VMEM((8, LANES), jnp.int32),
            pltpu.SMEM((8, LANES), jnp.int32),
            sems((2, chunks * parts)),
            sems((2, chunks * parts)),
            sems((3,)),
            sems((cols_n + rows_n - 2,)),
            sems((cols_n + rows_n,)),
            sems((cols_n + rows_n - 2,)),
            sems((cols_n + rows_n,)),
            sems((4,)),
            sems((4,)),
            sems((zs - 1,)),
            sems((zs,)),
            sems((zs - 1,)),
            sems((zs,)),
            sems((rows_n - 1,)),
            sems((rows_n,)),
            sems((4,)),
        ],
        compiler_params=pltpu.CompilerParams(
            collective_id=2, has_side_effects=True, vmem_limit_bytes=60 * MIB
        ),
    )(ids[0], counts[0], rows[0], counts[0], rows[1], counts[1], rows[2], counts[2], blocks, s_own)


def packed_kernel(codes, counts, p_pair, p_recv, s_own, s_recv, out, left, right, sem):
    near, s_near = p_pair.shape[0], s_own.shape[0]
    loads = [
        pltpu.make_async_copy(p_pair, left.at[pl.ds(0, near)], sem.at[0]),
        pltpu.make_async_copy(p_recv, left.at[pl.ds(near, p_recv.shape[0])], sem.at[1]),
        pltpu.make_async_copy(s_own, right.at[pl.ds(0, s_near)], sem.at[2]),
        pltpu.make_async_copy(s_recv, right.at[pl.ds(s_near, s_recv.shape[0])], sem.at[3]),
    ]
    for load in loads:
        load.start()
    for load in loads:
        load.wait()

    def slot(q, carry):
        def term(n, total):
            code = codes[q, n]
            return total + jnp.dot(
                left[lax.div(code, CODE)],
                right[lax.rem(code, CODE)],
                preferred_element_type=jnp.float32,
            )

        out[q] = lax.fori_loop(0, counts[0, q], term, jnp.zeros((128, 128), jnp.float32))
        return carry

    lax.fori_loop(0, out.shape[0], slot, 0)


def packed_product(codes, counts, p_pair, p_recv, s_own, s_recv):
    p_recv = p_recv.reshape(-1, 128, 128)
    s_recv = s_recv.reshape(-1, 128, 128)
    return pl.pallas_call(
        packed_kernel,
        out_shape=jax.ShapeDtypeStruct((codes.shape[0], 128, 128), jnp.float32),
        in_specs=[pl.BlockSpec(memory_space=pltpu.SMEM)] * 2
        + [pl.BlockSpec(memory_space=pl.ANY)] * 4,
        out_specs=pl.BlockSpec(memory_space=pltpu.VMEM),
        scratch_shapes=[
            pltpu.VMEM((p_pair.shape[0] + p_recv.shape[0], 128, 128), p_pair.dtype),
            pltpu.VMEM((s_own.shape[0] + s_recv.shape[0], 128, 128), s_own.dtype),
            pltpu.SemaphoreType.DMA((4,)),
        ],
        compiler_params=pltpu.CompilerParams(vmem_limit_bytes=40 * MIB),
    )(codes, counts, p_pair, p_recv, s_own, s_recv)


def blocks_kernel(rows_n, cols_n, parts, p_own, s_own, p_all, s_all, *sems):
    send, recv, pass_send, pass_recv, s_send, s_recv = sems
    row, col = lax.axis_index("row"), lax.axis_index("col")
    length = cols_n // 2
    z, core = lax.div(col, 2), lax.rem(col, 2)
    size = p_own.shape[0] // parts
    right, left = {"row": row, "col": col + 2}, {"row": row, "col": col - 2}
    partner = {"row": row, "col": z * 2 + 1 - core}
    column = [{"row": lax.rem(row + step, rows_n), "col": col} for step in range(1, rows_n)]
    has_right, has_left = z + 1 < length, z > 0

    barrier = pltpu.get_barrier_semaphore()

    def greet(device):
        pl.semaphore_signal(barrier, inc=1, device_id=device, device_id_type=MESH)

    greet(partner)
    for device in column:
        greet(device)

    @pl.when(has_right)
    def _():
        greet(right)

    @pl.when(has_left)
    def _():
        greet(left)

    pl.semaphore_wait(barrier, rows_n + jnp.where(has_right, 1, 0) + jnp.where(has_left, 1, 0))

    def remote(src, dst, send_sem, recv_sem, device):
        return pltpu.make_async_remote_copy(
            src_ref=src,
            dst_ref=dst,
            send_sem=send_sem,
            recv_sem=recv_sem,
            device_id=device,
            device_id_type=MESH,
        )

    def piece(source, lane, part):
        return p_all.at[source * 2 + lane, pl.ds(part * size, size)]

    def origin(way, step):
        return z - step if way == 0 else z + step

    def sent(way, step, part):
        where = piece(origin(way, step), core, part)
        src = p_own.at[pl.ds(part * size, size)] if step == 0 else where
        device = right if way == 0 else left
        return remote(src, where, send.at[way, step, part], recv.at[way, step, part], device)

    def passed(way, step, part):
        where = piece(origin(way, step), core, part)
        src = p_own.at[pl.ds(part * size, size)] if step == 0 else where
        return remote(
            src, where, pass_send.at[way, step, part], pass_recv.at[way, step, part], partner
        )

    def onward(way):
        return has_right if way == 0 else has_left

    def exists(way, step):
        return z >= step if way == 0 else z + step < length

    for part in range(parts):
        for way in range(2):
            pl.when(onward(way))(lambda way=way: sent(way, 0, part).start())
    s_sends = [
        remote(s_own, s_all.at[row], s_send.at[n], s_recv.at[n], device)
        for n, device in enumerate(column)
    ]
    for one in s_sends:
        one.start()
    for part in range(parts):
        passed(0, 0, part).start()
    for step in range(1, length):
        for part in range(parts):
            for way in range(2):

                @pl.when(exists(way, step))
                def _():
                    sent(way, step - 1, part).wait_recv()
                    passed(way, step, part).start()
                    if step < length - 1:
                        pl.when(onward(way))(lambda: sent(way, step, part).start())

    for part in range(parts):
        passed(0, 0, part).wait()
        for way in range(2):
            pl.when(onward(way))(lambda way=way: sent(way, 0, part).wait_send())
    for step in range(1, length):
        for part in range(parts):
            for way in range(2):

                @pl.when(exists(way, step))
                def _():
                    passed(way, step, part).wait()
                    if step < length - 1:
                        pl.when(onward(way))(lambda: sent(way, step, part).wait_send())

    for one in s_sends:
        one.wait()


def gather_blocks(p_own, s_own, rows_n, cols_n):
    parts = 4 if p_own.shape[0] % 4 == 0 else 1
    table = pltpu.SemaphoreType.DMA((2, cols_n // 2, parts))
    return pl.pallas_call(
        functools.partial(blocks_kernel, rows_n, cols_n, parts),
        out_shape=(
            jax.ShapeDtypeStruct((cols_n,) + p_own.shape, p_own.dtype),
            jax.ShapeDtypeStruct((rows_n,) + s_own.shape, s_own.dtype),
        ),
        in_specs=[pl.BlockSpec(memory_space=pl.ANY)] * 2,
        out_specs=[pl.BlockSpec(memory_space=pl.ANY)] * 2,
        scratch_shapes=[table] * 4 + [pltpu.SemaphoreType.DMA((rows_n - 1,))] * 2,
        compiler_params=pltpu.CompilerParams(collective_id=1, has_side_effects=True),
    )(p_own, s_own)


def product_kernel(rows_n, cols_n, codes, counts, p_own, s_own, p_all, s_all, out, left, right, sem):
    row, col = lax.axis_index("row"), lax.axis_index("col")
    p_max, s_max = p_own.shape[0], s_own.shape[0]
    base = rows_n * s_max
    loads = [pltpu.make_async_copy(p_own, left.at[pl.ds(col * p_max, p_max)], sem.at[0])]
    loads += [pltpu.make_async_copy(s_own, right.at[pl.ds(row * s_max, s_max)], sem.at[1])]
    for step in range(1, cols_n):
        at = lax.rem(col + step, cols_n)
        loads += [
            pltpu.make_async_copy(
                p_all.at[at], left.at[pl.ds(at * p_max, p_max)], sem.at[len(loads)]
            )
        ]
    for step in range(1, rows_n):
        at = lax.rem(row + step, rows_n)
        loads += [
            pltpu.make_async_copy(
                s_all.at[at], right.at[pl.ds(at * s_max, s_max)], sem.at[len(loads)]
            )
        ]
    for load in loads:
        load.start()
    for load in loads:
        load.wait()

    def slot(q, carry):
        def term(n, total):
            code = codes[q, n]
            return total + jnp.dot(
                left[lax.div(code, base)],
                right[lax.rem(code, base)],
                preferred_element_type=jnp.float32,
            )

        out[q] = lax.fori_loop(0, counts[q], term, jnp.zeros((128, 128), jnp.float32))
        return carry

    lax.fori_loop(0, out.shape[0], slot, 0)


def block_product(codes, counts, p_own, s_own, p_all, s_all):
    cols_n, p_max = p_all.shape[:2]
    rows_n, s_max = s_all.shape[:2]
    return pl.pallas_call(
        functools.partial(product_kernel, rows_n, cols_n),
        out_shape=jax.ShapeDtypeStruct((counts.shape[0], 128, 128), jnp.float32),
        in_specs=[pl.BlockSpec(memory_space=pltpu.SMEM)] * 2
        + [pl.BlockSpec(memory_space=pl.ANY)] * 4,
        out_specs=pl.BlockSpec(memory_space=pltpu.VMEM),
        scratch_shapes=[
            pltpu.VMEM((cols_n * p_max, 128, 128), p_all.dtype),
            pltpu.VMEM((rows_n * s_max, 128, 128), s_all.dtype),
            pltpu.SemaphoreType.DMA((cols_n + rows_n,)),
        ],
        compiler_params=pltpu.CompilerParams(vmem_limit_bytes=40 * MIB),
    )(codes, counts, p_own, s_own, p_all, s_all)


def match_lists(p_codes, s_codes, q_ids, q_live, tile_cols, span):
    cols_n, p_max = p_codes.shape
    rows_n, s_max = s_codes.shape
    q_row, q_col = q_ids // tile_cols, q_ids % tile_cols
    at = jnp.arange(tile_cols, dtype=jnp.int32)
    p_want = q_row[:, None] * tile_cols + at[None, :]
    p_hit = p_codes[None, :, None, :] == p_want[:, None, :, None]
    p_slot = jnp.arange(cols_n * p_max, dtype=jnp.int32).reshape(1, cols_n, 1, p_max)
    p_at = jnp.max(jnp.where(p_hit, p_slot, -1), axis=3)
    level = jnp.arange(span * tile_cols, dtype=jnp.int32).reshape(span, tile_cols)
    s_want = level[None] * tile_cols + q_col[:, None, None]
    s_hit = s_codes[None, None, :, None, :] == s_want[:, :, None, :, None]
    s_slot = jnp.arange(rows_n * s_max, dtype=jnp.int32).reshape(1, 1, rows_n, 1, s_max)
    s_at = jnp.max(jnp.where(s_hit, s_slot, -1), axis=4)
    p_at = p_at.reshape(q_ids.shape[0], -1)
    s_at = s_at.reshape(q_ids.shape[0], -1)
    depth = p_at.shape[1]
    match = (p_at >= 0) & (s_at >= 0) & q_live[:, None]
    code = jnp.where(match, p_at * (rows_n * s_max) + s_at, 0)
    order = jnp.arange(depth, dtype=jnp.int32)
    before = order[None, :, None] > order[None, None, :]
    rank = jnp.sum((before & match[:, None, :]).astype(jnp.int32), axis=2)
    rank = jnp.where(match, rank, -1)
    picked = rank[:, None, :] == order[None, :, None]
    codes = jnp.sum(jnp.where(picked, code[:, None, :], 0), axis=2)
    return codes, jnp.sum(match.astype(jnp.int32), axis=1)


def on_device(coeffs, p_slots, p_count, s_blocks, s_slots, s_count, q_slots, q_count):
    rows_n = lax.axis_size("row")
    cols_n = lax.axis_size("col")
    tile_cols = coeffs.shape[0] * rows_n // cols_n // 128
    p_ids, s_ids, q_ids = p_slots[0, 0], s_slots[0, 0], q_slots[0, 0]
    s_own = s_blocks[0, 0]
    p_max, s_max, q_max = p_ids.shape[0], s_ids.shape[0], q_ids.shape[0]

    def live(ids, count):
        return jnp.arange(ids.shape[0], dtype=jnp.int32) < count[0, 0]

    def whole(p_codes, s_codes, p_own):
        codes, counts = match_lists(
            p_codes, s_codes, q_ids, live(q_ids, q_count), tile_cols, cols_n // rows_n
        )
        p_all, s_all = gather_blocks(p_own, s_own, rows_n, cols_n)
        return block_product(codes, counts, p_own, s_own, p_all, s_all)

    if rows_n == 4 and tile_cols * cols_n == LANES and max(p_max, s_max, q_max) <= LANES // 2:
        counts = (p_count[0], q_count[0], s_count[0])
        p_own, p_pair, p_recv, s_recv, codes, pairs, over, meta = panel_density(
            (p_ids, q_ids, s_ids), counts, coeffs, s_own, rows_n, cols_n
        )

        def full():
            row, col = lax.axis_index("row"), lax.axis_index("col")
            p_codes = lax.dynamic_index_in_dim(meta, row, 0, False)[:, 0, :p_max]
            s_codes = lax.dynamic_index_in_dim(meta, col, 1, False)[:, 2, :s_max]
            return whole(p_codes, s_codes, p_own)

        def packed():
            return packed_product(codes, pairs, p_pair, p_recv, s_own, s_recv)

        product = lax.cond(jnp.max(over) > 0, full, packed)
    else:
        p_codes = lax.all_gather(jnp.where(live(p_ids, p_count), p_ids, -1), "col")
        s_codes = lax.all_gather(jnp.where(live(s_ids, s_count), s_ids, -1), "row")
        others = gather_rows(coeffs, rows_n, cols_n)
        p_own = density(p_ids, p_count[0], coeffs, others, rows_n, cols_n)
        product = whole(p_codes, s_codes, p_own)
    return (p_own.reshape(1, 1, p_max, 128, 128), product.reshape(1, 1, q_max, 128, 128))


def solution(mesh):
    return jax.shard_map(
        on_device,
        mesh=mesh,
        in_specs=(
            P("row", None),
            P("row", "col", None),
            P("row", "col"),
            P("row", "col", None, None, None),
            P("row", "col", None),
            P("row", "col"),
            P("row", "col", None),
            P("row", "col"),
        ),
        out_specs=(P("row", "col", None, None, None), P("row", "col", None, None, None)),
        check_vma=False,
    )
```

```python
import functools

import jax
import jax.numpy as jnp
from jax import lax
from jax.experimental import pallas as pl
from jax.experimental.pallas import tpu as pltpu
from jax.sharding import PartitionSpec as P

MESH = pl.DeviceIdType.MESH
MIB = 1 << 20
DEPTH = 3
BATCH = 8
LANES = 128
CODE = 512
PHASES = ((10, 4, 5, 30), (6, 4, 3, 20))
LAG = 2
S_CAP = 44


def rows_kernel(rows_n, cols_n, coeffs, out, send, recv):
    row, col = lax.axis_index("row"), lax.axis_index("col")
    sub = cols_n // rows_n
    height = out.shape[0]
    piece = height // rows_n
    half, share = lax.rem(col, sub), lax.div(col, sub)
    owner = lax.div(col, sub)
    targets = [
        {"row": lax.rem(row + step, rows_n), "col": row * sub + half} for step in range(1, rows_n)
    ]
    sources = [{"row": owner, "col": part * sub + half} for part in range(rows_n)]
    barrier = pltpu.get_barrier_semaphore()
    for device in targets:
        pl.semaphore_signal(barrier, inc=1, device_id=device, device_id_type=MESH)

    @pl.when(row != owner)
    def _():
        for device in sources:
            pl.semaphore_signal(barrier, inc=1, device_id=device, device_id_type=MESH)

    pl.semaphore_wait(barrier, rows_n - 1 + jnp.where(row != owner, rows_n, 0))

    def copy(step, part, device):
        start = half * height + share * piece
        return pltpu.make_async_remote_copy(
            src_ref=coeffs.at[pl.ds(pl.multiple_of(start, piece), piece)],
            dst_ref=out.at[pl.ds(pl.multiple_of(part * piece, piece), piece)],
            send_sem=send.at[step],
            recv_sem=recv.at[part],
            device_id=device,
            device_id_type=MESH,
        )

    sends = [copy(step, share, device) for step, device in enumerate(targets)]
    for one in sends:
        one.start()

    @pl.when(row != owner)
    def _():
        for part, device in enumerate(sources):
            copy(0, part, device).wait_recv()

    for one in sends:
        one.wait_send()


def gather_rows(coeffs, rows_n, cols_n):
    height = coeffs.shape[0] * rows_n // cols_n
    body = functools.partial(rows_kernel, rows_n, cols_n)
    sems = [pltpu.SemaphoreType.DMA((rows_n - 1,)), pltpu.SemaphoreType.DMA((rows_n,))]
    return pl.pallas_call(
        body,
        out_shape=jax.ShapeDtypeStruct((height, coeffs.shape[1]), coeffs.dtype),
        in_specs=[pl.BlockSpec(memory_space=pl.ANY)],
        out_specs=pl.BlockSpec(memory_space=pl.ANY),
        scratch_shapes=sems,
        compiler_params=pltpu.CompilerParams(collective_id=0, has_side_effects=True),
    )(coeffs)


def density_kernel(rows_n, cols_n, ids, count, coeffs, others, out, left, right, sem):
    row, col = lax.axis_index("row"), lax.axis_index("col")
    sub = cols_n // rows_n
    height = others.shape[0]
    tile_cols = height // 128
    load_left = pltpu.make_async_copy(coeffs, left, sem.at[0])
    load_left.start()
    here = row == lax.div(col, sub)
    start = pl.multiple_of(lax.rem(col, sub) * height, height)
    load_own = pltpu.make_async_copy(coeffs.at[pl.ds(start, height)], right, sem.at[1])
    load_other = pltpu.make_async_copy(others, right, sem.at[1])

    @pl.when(here)
    def _():
        load_own.start()

    @pl.when(jnp.logical_not(here))
    def _():
        load_other.start()

    live = count[0]
    load_left.wait()
    load_other.wait()

    def block(slot, carry):
        a = pl.multiple_of(lax.div(ids[slot], tile_cols) * 128, 128)
        b = pl.multiple_of(lax.rem(ids[slot], tile_cols) * 128, 128)
        raw = lax.dot_general(
            left[pl.ds(a, 128), :],
            right[pl.ds(b, 128), :],
            (((1,), (1,)), ((), ())),
            preferred_element_type=jnp.float32,
        )
        out[slot] = raw.astype(out.dtype)
        return carry

    def clear(slot, carry):
        out[slot] = jnp.zeros(out.shape[1:], out.dtype)
        return carry

    lax.fori_loop(0, live, block, 0)
    lax.fori_loop(live, out.shape[0], clear, 0)


def density(ids, count, coeffs, others, rows_n, cols_n):
    slots = ids.shape[0]
    return pl.pallas_call(
        functools.partial(density_kernel, rows_n, cols_n),
        out_shape=jax.ShapeDtypeStruct((slots, 128, 128), jnp.bfloat16),
        in_specs=[pl.BlockSpec(memory_space=pltpu.SMEM)] * 2
        + [pl.BlockSpec(memory_space=pl.ANY)] * 2,
        out_specs=pl.BlockSpec(memory_space=pltpu.VMEM),
        scratch_shapes=[
            pltpu.VMEM(coeffs.shape, coeffs.dtype),
            pltpu.VMEM(others.shape, coeffs.dtype),
            pltpu.SemaphoreType.DMA((2,)),
        ],
        compiler_params=pltpu.CompilerParams(vmem_limit_bytes=40 * MIB),
    )(ids, count, coeffs, others)


def nt(x, y, precision=None):
    return lax.dot_general(
        x, y, (((1,), (1,)), ((), ())), precision=precision, preferred_element_type=jnp.float32
    )


def nn(x, y, precision=None):
    return jnp.dot(x, y, precision=precision, preferred_element_type=jnp.float32)


def iota(shape, dim):
    return lax.broadcasted_iota(jnp.int32, shape, dim)


def onehot(codes, height, kind=jnp.bfloat16):
    hit = iota((height, LANES), 0) == codes
    return jnp.where(hit, 1.0, 0.0).astype(kind)


def flat(x):
    return jnp.minimum(x, 1.0).astype(jnp.bfloat16)


def panel_kernel(rows_n, cols_n, phases, depth, *refs):
    stages = len(phases)
    ids, count, p_row, p_live, q_row, q_live, s_row, s_live, coeffs, s_in = refs[:10]
    density, p_pair_out, s_recv, codes, counts, flags_out, meta_out = refs[10:17]
    p_recv = refs[17 : 17 + stages]
    refs = refs[17 + stages :]
    right = []
    for _, chunks, _, _ in phases:
        right.append(refs[:chunks])
        refs = refs[chunks:]
    p_pair, p_pack = refs[:stages], refs[stages : 2 * stages]
    (
        left, total, s_pair, s_pack, meta, flags,
        p_dense, q_dense, q_wide, s_dense, p_need, p_rank, s_need, s_rank, lists, lists_s,
        send, recv, sem, meta_send, meta_recv, flag_send, flag_recv,
        pair_send, pair_recv, p_send, p_got, pass_send, pass_recv,
        s_send, s_got, s_pass_send, s_pass_recv, s_swap, done,
    ) = refs[2 * stages :]
    row, col = lax.axis_index("row"), lax.axis_index("col")
    slots = ids.shape[0]
    sub = cols_n // rows_n
    zs = cols_n // 2
    tile_rows = left.shape[0]
    tile_cols = sum(phase[0] for phase in phases)
    bits = tile_cols.bit_length() - 1
    caps = [phase[3] for phase in phases]
    starts = [sum(phase[0] for phase in phases[:f]) for f in range(stages)]
    bases = [2 * slots + zs * sum(caps[:f]) for f in range(stages)]
    s_cap = s_recv.shape[1] * s_recv.shape[2]
    z, core = lax.div(col, 2), lax.rem(col, 2)
    owner = lax.div(col, sub)
    first = lax.rem(col, sub) * tile_cols
    y, x = lax.div(row, 2), lax.rem(row, 2)
    dy = lax.rem(y + lax.div(owner, 2), 2)
    dx = lax.rem(x + lax.rem(owner, 2), 2)
    along_x, along_y = y * 2 + 1 - x, (1 - y) * 2 + x
    is_source = row == owner
    sends = [jnp.logical_or(dx == 1, dy == 0), jnp.logical_or(dx == 0, dy == 1)]
    following = [
        jnp.where(dx == dy, along_x, along_y),
        jnp.where(dx == dy, along_y, along_x),
    ]
    pieces = [(f, k) for f in range(stages) for k in range(phases[f][1])]
    steps = [(f, k, part) for f, k in pieces for part in range(phases[f][2])]
    partner = {"row": row, "col": z * 2 + 1 - core}
    row_mates = [{"row": row, "col": lax.rem(col + n, cols_n)} for n in range(1, cols_n)]
    col_mates = [{"row": lax.rem(row + n, rows_n), "col": col} for n in range(1, rows_n)]

    def remote(src, dst, send_sem, recv_sem, device):
        return pltpu.make_async_remote_copy(
            src_ref=src,
            dst_ref=dst,
            send_sem=send_sem,
            recv_sem=recv_sem,
            device_id=device,
            device_id_type=MESH,
        )

    def area(way, f, part):
        size = phases[f][0] // (2 * phases[f][2])
        return (way * phases[f][2] + part) * size, size

    def load(way, f, k, part):
        at, size = area(way, f, part)
        wide = right[f][k].shape[2]
        return pltpu.make_async_copy(
            coeffs.at[pl.ds(first + starts[f] + at, size), :, pl.ds(k * wide, wide)],
            right[f][k].at[pl.ds(at, size)],
            recv.at[way, steps.index((f, k, part))],
        )

    def copy(way, f, k, part):
        where = right[f][k].at[pl.ds(*area(way, f, part))]
        device = {"row": following[way], "col": col}
        at = steps.index((f, k, part))
        return remote(where, where, send.at[way, at], recv.at[way, at], device)

    @pl.when(is_source)
    def _():
        for step in steps:
            for way in range(2):
                load(way, *step).start()

    load_left = pltpu.make_async_copy(coeffs, left, sem.at[0])
    load_s = pltpu.make_async_copy(s_in, s_pair.at[pl.ds(core * slots, slots)], sem.at[1])
    load_left.start()
    load_s.start()

    mine = jnp.full((8, LANES), -1, jnp.int32)
    lane = iota((8, LANES), 1)
    height = iota((8, LANES), 0)
    for at, (codes_in, live_in) in enumerate(((p_row, p_live), (q_row, q_live), (s_row, s_live))):
        keep = jnp.logical_and(height == at, lane < live_in[0])
        mine = jnp.where(keep, codes_in[...], mine)
    meta[row, col] = mine

    barrier = pltpu.get_barrier_semaphore()
    for device in row_mates + col_mates:
        pl.semaphore_signal(barrier, inc=1, device_id=device, device_id_type=MESH)
    pl.semaphore_wait(barrier, len(row_mates) + len(col_mates))

    def along_row(table, send_sem, recv_sem, source, n):
        where = table.at[row, source]
        return remote(where, where, send_sem.at[n], recv_sem.at[source], row_mates[n])

    def along_col(table, send_sem, recv_sem, source, n):
        where = table.at[source]
        at = len(row_mates) + n
        return remote(where, where, send_sem.at[at], recv_sem.at[cols_n + source], col_mates[n])

    def spread(table, send_sem, recv_sem):
        def first_half():
            for n in range(cols_n - 1):
                along_row(table, send_sem, recv_sem, col, n).start()

        def second_half():
            for n in range(cols_n - 1):
                source = lax.rem(col + cols_n - 1 - n, cols_n)
                along_row(table, send_sem, recv_sem, source, n).wait_recv()
            for n in range(rows_n - 1):
                along_col(table, send_sem, recv_sem, row, n).start()

        def last():
            for n in range(rows_n - 1):
                source = lax.rem(row + rows_n - 1 - n, rows_n)
                along_col(table, send_sem, recv_sem, source, n).wait_recv()
            for n in range(cols_n - 1):
                along_row(table, send_sem, recv_sem, col, n).wait_send()
            for n in range(rows_n - 1):
                along_col(table, send_sem, recv_sem, row, n).wait_send()

        return first_half, second_half, last

    meta_steps = spread(meta, meta_send, meta_recv)
    flag_steps = spread(flags, flag_send, flag_recv)
    meta_steps[0]()

    def code(at, r, c):
        return meta[r, c][at : at + 1]

    def split(at, r, c):
        value = code(at, r, c)
        return value >> bits, c * tile_cols + (value & (tile_cols - 1))

    def split_s(r, c):
        value = code(2, r, c)
        local = value >> bits
        k = (r + rows_n * (local >> bits)) * tile_cols + (local & (tile_cols - 1))
        return k, c * tile_cols + (value & (tile_cols - 1))

    lanes = iota((1, LANES), 1)
    ahead = jnp.where(iota((LANES, LANES), 0) <= iota((LANES, LANES), 1), 1.0, 0.0)
    ahead = ahead.astype(jnp.bfloat16)
    exact = lax.Precision.HIGHEST

    def dense_rows(r):
        p_sum = jnp.zeros((LANES, tile_rows), jnp.float32)
        q_sum = jnp.zeros((LANES, tile_rows), jnp.float32)
        q_turn = jnp.zeros((tile_rows, LANES), jnp.float32)
        for c in range(cols_n):
            a, k = split(0, r, c)
            p_sum += nt(onehot(k, LANES), onehot(a, tile_rows))
            a, k = split(1, r, c)
            at_row, at_col = onehot(a, tile_rows), onehot(k, LANES)
            q_sum += nt(at_col, at_row)
            q_turn += nt(at_row, at_col)
        p_dense[r] = p_sum.astype(jnp.bfloat16)
        q_dense[r] = q_sum.astype(jnp.bfloat16)
        q_wide[r] = q_turn.astype(jnp.bfloat16)

    def dense_s():
        s_sum = jnp.zeros((LANES, LANES), jnp.float32)
        for r in range(rows_n):
            for c in range(cols_n):
                k, j = split_s(r, c)
                s_sum += nt(onehot(k, LANES), onehot(j, LANES))
        s_dense[...] = s_sum.astype(jnp.bfloat16)

    def ranked(need, rank, size):
        plain = nn(need[:size].astype(jnp.bfloat16), ahead)
        before = pltpu.roll(jnp.max(plain, axis=1, keepdims=True) + jnp.zeros_like(plain), 1, 0)
        odd = iota(plain.shape, 0) % 2 == 1
        rank[:size] = plain + jnp.where(odd, before, 0.0)

    def p_at(f, d, c):
        return (f * zs + d) * cols_n + c

    def s_at(r, source, half):
        return (r * rows_n + source) * 2 + half

    def need_p():
        wants = []
        for d in range(zs):
            group = lax.broadcasted_iota(jnp.int32, (tile_rows, LANES), 1) // (2 * tile_cols)
            part = jnp.where(group == d, q_wide[row].astype(jnp.float32), 0.0)
            wants.append(flat(nt(s_dense[...], part.astype(jnp.bfloat16))))
        for c in range(cols_n):
            a, k = split(0, row, c)
            at_row, at_k = onehot(a, tile_rows), onehot(k, LANES, jnp.float32)
            b = k - c * tile_cols
            for d in range(zs):
                hit = jnp.sum(nn(wants[d], at_row) * at_k, axis=0, keepdims=True)
                hit = jnp.minimum(hit, 1.0)
                for f in range(stages):
                    inside = jnp.logical_and(b >= starts[f], b < starts[f] + phases[f][0])
                    p_need[pl.ds(p_at(f, d, c), 1)] = jnp.where(inside, hit, 0.0)
        ranked(p_need, p_rank, stages * zs * cols_n)

    def need_s():
        for r in range(rows_n):
            wants = flat(nt(q_dense[r], p_dense[r]))
            for source in range(rows_n):
                for half in range(2):
                    k, j = split_s(source, z * 2 + half)
                    hit = nn(wants, onehot(k, LANES)) * onehot(j, LANES, jnp.float32)
                    hit = jnp.sum(hit, axis=0, keepdims=True)
                    s_need[pl.ds(s_at(r, source, half), 1)] = jnp.minimum(hit, 1.0)
        ranked(s_need, s_rank, rows_n * rows_n * 2)

    def picks(need, rank, base):
        chosen = jnp.logical_and(rank == (iota((LANES, LANES), 0) + 1).astype(jnp.float32), need > 0)
        chosen = jnp.where(chosen, 1.0, 0.0).astype(jnp.bfloat16)
        values = (base + lane).astype(jnp.float32).astype(jnp.bfloat16)
        return nt(values, chosen)

    def picked(need, rank, at):
        entry = jnp.zeros((8, LANES), jnp.float32)
        for half in range(2):
            row_at = pl.ds(at + half, 1)
            entry += picks(need[row_at], rank[row_at], half * slots)
        return entry

    def make_lists():
        for n in range(lists.shape[0] // 8):
            made = jnp.zeros((8, LANES), jnp.float32)
            for at in range(8):
                f, d = divmod(n * 8 + at, zs)
                r = n * 8 + at - stages * zs
                if f < stages:
                    entry = picked(p_need, p_rank, p_at(f, d, z * 2))
                elif r < rows_n:
                    entry = picked(s_need, s_rank, s_at(r, row, 0))
                else:
                    continue
                made = jnp.where(height == at, entry, made)
            lists[n * 8 : n * 8 + 8] = made.astype(jnp.int32)
        load_lists.start()

    def make_flags():
        over = jnp.zeros((1, 1), jnp.float32)
        for d in range(zs):
            for f in range(stages):
                most = jnp.max(p_rank[pl.ds(p_at(f, z, d * 2 + 1), 1)], axis=1, keepdims=True)
                over = jnp.maximum(over, jnp.where(d == z, 0.0, most - caps[f]))
        for r in range(rows_n):
            most = jnp.max(s_rank[pl.ds(s_at(row, r, 1), 1)], axis=1, keepdims=True)
            over = jnp.maximum(over, jnp.where(r == row, 0.0, most - s_cap))
        flags[row, col] = (over + jnp.zeros((8, LANES), jnp.float32)).astype(jnp.int32)
        flag_steps[0]()

    def make_codes():
        p_sum = jnp.zeros((tile_rows, LANES), jnp.float32)
        for c in range(cols_n):
            a, k = split(0, row, c)
            place = (c % 2 * slots + 1 + lanes).astype(jnp.float32)
            far = jnp.zeros((1, LANES), jnp.float32)
            for f in range(stages):
                at = pl.ds(p_at(f, z, c), 1)
                spot = bases[f] + c // 2 * caps[f] + p_rank[at]
                far = far + jnp.where(p_need[at] > 0, spot, 0.0)
            place = jnp.where(c // 2 == z, place, far)
            p_sum += nt(
                onehot(a, tile_rows, jnp.float32) * place, onehot(k, LANES, jnp.float32), exact
            )
        s_sum = jnp.zeros((LANES, LANES), jnp.float32)
        for r in range(rows_n):
            k, j = split_s(r, col)
            at = pl.ds(s_at(row, r, core), 1)
            far = jnp.where(s_need[at] > 0, slots + r * s_cap + s_rank[at], 0.0)
            place = jnp.where(r == row, (1 + lanes).astype(jnp.float32), far)
            s_sum += nt(onehot(j, LANES, jnp.float32) * place, onehot(k, LANES, jnp.float32), exact)
        a, j = split(1, row, col)
        unit = onehot(lanes, LANES)
        q_row_hot = nt(unit, onehot(a, tile_rows))[:slots]
        q_col_hot = nt(unit, onehot(j, LANES))[:slots]
        p_for = nn(q_row_hot, p_sum, exact)
        s_for = nn(q_col_hot, s_sum, exact)
        match = jnp.where(jnp.logical_and(p_for > 0, s_for > 0), 1.0, 0.0)
        value = (p_for - 1) * CODE + (s_for - 1)
        rank = nn(match.astype(jnp.bfloat16), ahead) * match
        counts[...] = nt(
            jnp.ones((8, LANES), jnp.bfloat16), match.astype(jnp.bfloat16)
        ).astype(jnp.int32)

        def place_one(n, made):
            here = jnp.where(rank == (n + 1).astype(jnp.float32), value, 0.0)
            here = jnp.sum(here, axis=1, keepdims=True)
            return jnp.where(iota(made.shape, 1) == n, here, made)

        made = jnp.zeros((slots, LANES), jnp.float32)
        made = lax.fori_loop(0, LANES, place_one, made, unroll=8)
        codes[...] = made.astype(jnp.int32)

    load_lists = pltpu.make_async_copy(lists, lists_s, sem.at[2])

    groups = 4
    group = slots // groups

    def pair_copy(f, n, half):
        where = p_pair[f].at[pl.ds(half * slots + n * group, group)]
        return remote(where, where, pair_send.at[f, n], pair_recv.at[f, n], partner)

    def s_pair_copy(half):
        where = s_pair.at[pl.ds(half * slots, slots)]
        return remote(where, where, s_swap.at[0], s_swap.at[1], partner)

    def chip(n):
        return lax.rem(z + n + 1, zs)

    def p_copy(f, n):
        device = {"row": row, "col": chip(n) * 2 + core}
        where = p_recv[f].at[z, core]
        return remote(p_pack[f].at[n], where, p_send.at[f, n], p_got.at[f, z], device)

    def p_arrival(f, n):
        where = p_recv[f].at[chip(n), core]
        return remote(p_pack[f].at[n], where, p_send.at[f, n], p_got.at[f, chip(n)], partner)

    def p_pass(f, n, half):
        where = p_recv[f].at[chip(n), half]
        return remote(where, where, pass_send.at[f, n], pass_recv.at[f, chip(n)], partner)

    def s_copy(n):
        where = s_recv.at[row, core]
        return remote(s_pack.at[n], where, s_send.at[n], s_got.at[row], col_mates[n])

    def s_arrival(n):
        source = col_mates[n]["row"]
        where = s_recv.at[source, core]
        return remote(s_pack.at[n], where, s_send.at[n], s_got.at[source], partner)

    def s_pass(n, half):
        source = col_mates[n]["row"]
        where = s_recv.at[source, half]
        return remote(where, where, s_pass_send.at[n], s_pass_recv.at[source], partner)

    def pack_p(f):
        for n in range(groups):
            pair_copy(f, n, 1 - core).wait_recv()
        half = caps[f] // 2
        for n in range(zs - 1):

            def fill(t, carry, n=n):
                at = lists_s[f * zs + chip(n), core * half + t]
                p_pack[f][n, t] = p_pair[f][jnp.clip(at, 0, 2 * slots - 1)]
                return carry

            lax.fori_loop(0, half, fill, 0, unroll=5)
            if f == stages - 1 or n == 0:
                p_copy(f, n).start()

    def pack_s():
        s_pair_copy(1 - core).wait_recv()
        half = s_cap // 2
        for n in range(rows_n - 1):

            def fill(t, carry, n=n):
                at = lists_s[stages * zs + col_mates[n]["row"], core * half + t]
                s_pack[n, t] = s_pair[jnp.clip(at, 0, 2 * slots - 1)]
                return carry

            lax.fori_loop(0, half, fill, 0, unroll=2)

    def start_swap():
        load_s.wait()
        s_pair_copy(core).start()

    ready = phases[0][1]
    idle = [lambda: None]
    ready = phases[0][1]
    work = {
        0: [meta_steps[1]] + idle * 3 + [start_swap],
        1: [meta_steps[2]] + [functools.partial(dense_rows, r) for r in range(rows_n)],
        2: [dense_s, idle[0], need_p],
        3: [need_s, idle[0], make_lists],
        ready: [load_lists.wait, lambda: pack_p(0), make_flags],
        ready + 1: [p_copy(0, 1).start, flag_steps[1], make_codes],
        ready + 2: [flag_steps[2], idle[0], pack_s],
        ready + 3: [p_copy(0, 2).start],
    }

    def relay(n, part):
        f, k = pieces[n]
        now = steps.index((f, k, part))
        for way in range(2):

            @pl.when(sends[way])
            def _():
                copy(way, f, k, part).wait_recv()
                if now >= depth:
                    copy(way, *steps[now - depth]).wait_send()
                copy(way, f, k, part).start()

    for n in range(LAG):
        for part in range(phases[pieces[n][0]][2]):
            relay(n, part)
    load_left.wait()
    for n, (f, k) in enumerate(pieces):
        for way in range(2):

            @pl.when(jnp.logical_not(sends[way]))
            def _():
                for part in range(phases[f][2]):
                    copy(way, f, k, part).wait_recv()

        if n == len(pieces) - 1:
            for one in range(rows_n - 1):
                s_copy(one).start()
        wide = right[f][k].shape[2]
        ends = k == phases[f][1] - 1

        def blocks(step, carry, f=f, k=k, wide=wide, ends=ends):
            slot = [step * BATCH + one for one in range(BATCH)]
            b = [(ids[at] & (tile_cols - 1)) - starts[f] for at in slot]
            raw = [
                lax.dot_general(
                    left[ids[at] >> bits, :, pl.ds(k * wide, wide)],
                    right[f][k][jnp.clip(where, 0, phases[f][0] - 1)],
                    (((1,), (1,)), ((), ())),
                    preferred_element_type=jnp.float32,
                )
                for at, where in zip(slot, b)
            ]
            if k > 0:
                raw = [one + total[at] for one, at in zip(raw, slot)]
            if not ends:
                for one, at in zip(raw, slot):
                    total[at] = one
                return carry
            made = []
            for one, at, where in zip(raw, slot, b):
                inside = jnp.logical_and(where >= 0, where < phases[f][0])
                inside = jnp.logical_and(inside, at < count[0])
                other = 0.0
                if f > 0:
                    other = p_pair[f - 1][core * slots + at].astype(jnp.float32)
                made.append(jnp.where(inside, one, other).astype(p_pair[f].dtype))
            for one, at in zip(made, slot):
                p_pair[f][core * slots + at] = one
            return carry

        todo = list(work.get(n, []))
        later = n + LAG
        if later < len(pieces):
            pulls = [functools.partial(relay, later, p) for p in range(phases[pieces[later][0]][2])]
        else:
            pulls = []
        turns = groups if ends else max(len(pulls), len(todo), 1)
        batches = slots // BATCH
        for turn in range(turns):
            if turn < len(pulls):
                pulls[turn]()
            low, high = batches * turn // turns, batches * (turn + 1) // turns
            lax.fori_loop(low, high, blocks, 0)
            if ends:
                pair_copy(f, turn, core).start()
            if turn < len(todo):
                todo[turn]()
        for one in pulls[turns:] + todo[turns:]:
            one()

    final = p_pair[-1]
    density_out = pltpu.make_async_copy(final.at[pl.ds(core * slots, slots)], density, done.at[0])
    density_out.start()
    pack_p(stages - 1)
    pair_out = pltpu.make_async_copy(final, p_pair_out, done.at[1])
    flags_go = pltpu.make_async_copy(flags, flags_out, done.at[2])
    meta_go = pltpu.make_async_copy(meta, meta_out, done.at[3])
    for one in (pair_out, flags_go, meta_go):
        one.start()
    for way in range(2):

        @pl.when(sends[way])
        def _():
            for step in steps[-depth:]:
                copy(way, *step).wait_send()

    s_pair_copy(core).wait_send()
    for f in range(stages):
        for n in range(groups):
            pair_copy(f, n, core).wait_send()
    for f in range(stages):
        if f == stages - 1:
            for n in range(rows_n - 1):
                s_arrival(n).wait_recv()
                s_pass(n, core).start()
        for n in range(zs - 1):
            p_arrival(f, n).wait_recv()
            p_pass(f, n, core).start()
    for n in range(rows_n - 1):
        s_pass(n, 1 - core).wait_recv()
        s_pass(n, core).wait_send()
        s_copy(n).wait_send()
    for f in range(stages):
        for n in range(zs - 1):
            p_pass(f, n, 1 - core).wait_recv()
            p_pass(f, n, core).wait_send()
            p_copy(f, n).wait_send()
    for one in (density_out, pair_out, flags_go, meta_go):
        one.wait()


def panel_density(ids, counts, coeffs, s_own, rows_n, cols_n):
    slots = ids[0].shape[0]
    orbitals = coeffs.shape[1]
    blocks = coeffs.reshape(-1, 128, orbitals)
    tile_rows = blocks.shape[0]
    zs = cols_n // 2
    stages = len(PHASES)
    kind = coeffs.dtype
    block = (128, 128)
    smem, vmem = pl.BlockSpec(memory_space=pltpu.SMEM), pl.BlockSpec(memory_space=pltpu.VMEM)
    anywhere = pl.BlockSpec(memory_space=pl.ANY)
    rows = [jnp.pad(one[None], ((0, 0), (0, LANES - slots)), constant_values=-1) for one in ids]
    table = (rows_n, cols_n, 8, LANES)
    sems = pltpu.SemaphoreType.DMA
    steps = sum(chunks * parts for _, chunks, parts, _ in PHASES)
    p_rows, s_rows = stages * zs * cols_n + 8, rows_n * rows_n * 2 + 8
    list_rows = -(-(stages * zs + rows_n) // 8) * 8
    mates = cols_n + rows_n - 2
    panels = [
        pltpu.VMEM((wide, 128, orbitals // chunks), kind)
        for wide, chunks, _, _ in PHASES
        for _ in range(chunks)
    ]
    return pl.pallas_call(
        functools.partial(panel_kernel, rows_n, cols_n, PHASES, DEPTH),
        out_shape=[
            jax.ShapeDtypeStruct((slots,) + block, kind),
            jax.ShapeDtypeStruct((2 * slots,) + block, kind),
            jax.ShapeDtypeStruct((rows_n, 2, S_CAP // 2) + block, kind),
            jax.ShapeDtypeStruct((slots, LANES), jnp.int32),
            jax.ShapeDtypeStruct((8, slots), jnp.int32),
            jax.ShapeDtypeStruct(table, jnp.int32),
            jax.ShapeDtypeStruct(table, jnp.int32),
        ]
        + [jax.ShapeDtypeStruct((zs, 2, cap // 2) + block, kind) for _, _, _, cap in PHASES],
        in_specs=[smem, smem] + [vmem, smem] * 3 + [anywhere] * 2,
        out_specs=[anywhere] * 3 + [vmem] * 2 + [anywhere] * (2 + stages),
        scratch_shapes=panels
        + [pltpu.VMEM((2 * slots,) + block, kind)] * stages
        + [pltpu.VMEM((zs - 1, cap // 2) + block, kind) for _, _, _, cap in PHASES]
        + [
            pltpu.VMEM(blocks.shape, kind),
            pltpu.VMEM((slots,) + block, jnp.float32),
            pltpu.VMEM((2 * slots,) + block, kind),
            pltpu.VMEM((rows_n - 1, S_CAP // 2) + block, kind),
            pltpu.VMEM(table, jnp.int32),
            pltpu.VMEM(table, jnp.int32),
            pltpu.VMEM((rows_n, LANES, tile_rows), jnp.bfloat16),
            pltpu.VMEM((rows_n, LANES, tile_rows), jnp.bfloat16),
            pltpu.VMEM((rows_n, tile_rows, LANES), jnp.bfloat16),
            pltpu.VMEM((LANES, LANES), jnp.bfloat16),
            pltpu.VMEM((p_rows, LANES), jnp.float32),
            pltpu.VMEM((p_rows, LANES), jnp.float32),
            pltpu.VMEM((s_rows, LANES), jnp.float32),
            pltpu.VMEM((s_rows, LANES), jnp.float32),
            pltpu.VMEM((list_rows, LANES), jnp.int32),
            pltpu.SMEM((list_rows, LANES), jnp.int32),
            sems((2, steps)),
            sems((2, steps)),
            sems((3,)),
            sems((mates,)),
            sems((cols_n + rows_n,)),
            sems((mates,)),
            sems((cols_n + rows_n,)),
            sems((stages, 4)),
            sems((stages, 4)),
            sems((stages, zs - 1)),
            sems((stages, zs)),
            sems((stages, zs - 1)),
            sems((stages, zs)),
            sems((rows_n - 1,)),
            sems((rows_n,)),
            sems((rows_n - 1,)),
            sems((rows_n,)),
            sems((2,)),
            sems((4,)),
        ],
        compiler_params=pltpu.CompilerParams(
            collective_id=2, has_side_effects=True, vmem_limit_bytes=60 * MIB
        ),
    )(ids[0], counts[0], rows[0], counts[0], rows[1], counts[1], rows[2], counts[2], blocks, s_own)


def packed_kernel(codes, counts, *refs):
    sources, (out, left, right, sem) = refs[:-4], refs[-4:]
    loads = []
    for target, group in ((left, sources[:-2]), (right, sources[-2:])):
        at = 0
        for source in group:
            where = target.at[pl.ds(at, source.shape[0])]
            loads.append(pltpu.make_async_copy(source, where, sem.at[len(loads)]))
            at += source.shape[0]
    for load in loads:
        load.start()
    for load in loads:
        load.wait()

    def slot(q, carry):
        def term(n, total):
            code = codes[q, n]
            return total + jnp.dot(
                left[lax.div(code, CODE)],
                right[lax.rem(code, CODE)],
                preferred_element_type=jnp.float32,
            )

        out[q] = lax.fori_loop(0, counts[0, q], term, jnp.zeros((128, 128), jnp.float32))
        return carry

    lax.fori_loop(0, out.shape[0], slot, 0)


def packed_product(codes, counts, p_parts, s_parts):
    p_parts = [part.reshape(-1, 128, 128) for part in p_parts]
    s_parts = [part.reshape(-1, 128, 128) for part in s_parts]
    sizes = [sum(part.shape[0] for part in parts) for parts in (p_parts, s_parts)]
    kind = s_parts[0].dtype
    many = len(p_parts) + len(s_parts)
    return pl.pallas_call(
        packed_kernel,
        out_shape=jax.ShapeDtypeStruct((codes.shape[0], 128, 128), jnp.float32),
        in_specs=[pl.BlockSpec(memory_space=pltpu.SMEM)] * 2
        + [pl.BlockSpec(memory_space=pl.ANY)] * many,
        out_specs=pl.BlockSpec(memory_space=pltpu.VMEM),
        scratch_shapes=[pltpu.VMEM((size, 128, 128), kind) for size in sizes]
        + [pltpu.SemaphoreType.DMA((many,))],
        compiler_params=pltpu.CompilerParams(vmem_limit_bytes=40 * MIB),
    )(codes, counts, *p_parts, *s_parts)


def blocks_kernel(rows_n, cols_n, parts, p_own, s_own, p_all, s_all, *sems):
    send, recv, pass_send, pass_recv, s_send, s_recv = sems
    row, col = lax.axis_index("row"), lax.axis_index("col")
    length = cols_n // 2
    z, core = lax.div(col, 2), lax.rem(col, 2)
    size = p_own.shape[0] // parts
    right, left = {"row": row, "col": col + 2}, {"row": row, "col": col - 2}
    partner = {"row": row, "col": z * 2 + 1 - core}
    column = [{"row": lax.rem(row + step, rows_n), "col": col} for step in range(1, rows_n)]
    has_right, has_left = z + 1 < length, z > 0

    barrier = pltpu.get_barrier_semaphore()

    def greet(device):
        pl.semaphore_signal(barrier, inc=1, device_id=device, device_id_type=MESH)

    greet(partner)
    for device in column:
        greet(device)

    @pl.when(has_right)
    def _():
        greet(right)

    @pl.when(has_left)
    def _():
        greet(left)

    pl.semaphore_wait(barrier, rows_n + jnp.where(has_right, 1, 0) + jnp.where(has_left, 1, 0))

    def remote(src, dst, send_sem, recv_sem, device):
        return pltpu.make_async_remote_copy(
            src_ref=src,
            dst_ref=dst,
            send_sem=send_sem,
            recv_sem=recv_sem,
            device_id=device,
            device_id_type=MESH,
        )

    def piece(source, lane, part):
        return p_all.at[source * 2 + lane, pl.ds(part * size, size)]

    def origin(way, step):
        return z - step if way == 0 else z + step

    def sent(way, step, part):
        where = piece(origin(way, step), core, part)
        src = p_own.at[pl.ds(part * size, size)] if step == 0 else where
        device = right if way == 0 else left
        return remote(src, where, send.at[way, step, part], recv.at[way, step, part], device)

    def passed(way, step, part):
        where = piece(origin(way, step), core, part)
        src = p_own.at[pl.ds(part * size, size)] if step == 0 else where
        return remote(
            src, where, pass_send.at[way, step, part], pass_recv.at[way, step, part], partner
        )

    def onward(way):
        return has_right if way == 0 else has_left

    def exists(way, step):
        return z >= step if way == 0 else z + step < length

    for part in range(parts):
        for way in range(2):
            pl.when(onward(way))(lambda way=way: sent(way, 0, part).start())
    s_sends = [
        remote(s_own, s_all.at[row], s_send.at[n], s_recv.at[n], device)
        for n, device in enumerate(column)
    ]
    for one in s_sends:
        one.start()
    for part in range(parts):
        passed(0, 0, part).start()
    for step in range(1, length):
        for part in range(parts):
            for way in range(2):

                @pl.when(exists(way, step))
                def _():
                    sent(way, step - 1, part).wait_recv()
                    passed(way, step, part).start()
                    if step < length - 1:
                        pl.when(onward(way))(lambda: sent(way, step, part).start())

    for part in range(parts):
        passed(0, 0, part).wait()
        for way in range(2):
            pl.when(onward(way))(lambda way=way: sent(way, 0, part).wait_send())
    for step in range(1, length):
        for part in range(parts):
            for way in range(2):

                @pl.when(exists(way, step))
                def _():
                    passed(way, step, part).wait()
                    if step < length - 1:
                        pl.when(onward(way))(lambda: sent(way, step, part).wait_send())

    for one in s_sends:
        one.wait()


def gather_blocks(p_own, s_own, rows_n, cols_n):
    parts = 4 if p_own.shape[0] % 4 == 0 else 1
    table = pltpu.SemaphoreType.DMA((2, cols_n // 2, parts))
    return pl.pallas_call(
        functools.partial(blocks_kernel, rows_n, cols_n, parts),
        out_shape=(
            jax.ShapeDtypeStruct((cols_n,) + p_own.shape, p_own.dtype),
            jax.ShapeDtypeStruct((rows_n,) + s_own.shape, s_own.dtype),
        ),
        in_specs=[pl.BlockSpec(memory_space=pl.ANY)] * 2,
        out_specs=[pl.BlockSpec(memory_space=pl.ANY)] * 2,
        scratch_shapes=[table] * 4 + [pltpu.SemaphoreType.DMA((rows_n - 1,))] * 2,
        compiler_params=pltpu.CompilerParams(collective_id=1, has_side_effects=True),
    )(p_own, s_own)


def product_kernel(rows_n, cols_n, codes, counts, p_own, s_own, p_all, s_all, out, left, right, sem):
    row, col = lax.axis_index("row"), lax.axis_index("col")
    p_max, s_max = p_own.shape[0], s_own.shape[0]
    base = rows_n * s_max
    loads = [pltpu.make_async_copy(p_own, left.at[pl.ds(col * p_max, p_max)], sem.at[0])]
    loads += [pltpu.make_async_copy(s_own, right.at[pl.ds(row * s_max, s_max)], sem.at[1])]
    for step in range(1, cols_n):
        at = lax.rem(col + step, cols_n)
        loads += [
            pltpu.make_async_copy(
                p_all.at[at], left.at[pl.ds(at * p_max, p_max)], sem.at[len(loads)]
            )
        ]
    for step in range(1, rows_n):
        at = lax.rem(row + step, rows_n)
        loads += [
            pltpu.make_async_copy(
                s_all.at[at], right.at[pl.ds(at * s_max, s_max)], sem.at[len(loads)]
            )
        ]
    for load in loads:
        load.start()
    for load in loads:
        load.wait()

    def slot(q, carry):
        def term(n, total):
            code = codes[q, n]
            return total + jnp.dot(
                left[lax.div(code, base)],
                right[lax.rem(code, base)],
                preferred_element_type=jnp.float32,
            )

        out[q] = lax.fori_loop(0, counts[q], term, jnp.zeros((128, 128), jnp.float32))
        return carry

    lax.fori_loop(0, out.shape[0], slot, 0)


def block_product(codes, counts, p_own, s_own, p_all, s_all):
    cols_n, p_max = p_all.shape[:2]
    rows_n, s_max = s_all.shape[:2]
    return pl.pallas_call(
        functools.partial(product_kernel, rows_n, cols_n),
        out_shape=jax.ShapeDtypeStruct((counts.shape[0], 128, 128), jnp.float32),
        in_specs=[pl.BlockSpec(memory_space=pltpu.SMEM)] * 2
        + [pl.BlockSpec(memory_space=pl.ANY)] * 4,
        out_specs=pl.BlockSpec(memory_space=pltpu.VMEM),
        scratch_shapes=[
            pltpu.VMEM((cols_n * p_max, 128, 128), p_all.dtype),
            pltpu.VMEM((rows_n * s_max, 128, 128), s_all.dtype),
            pltpu.SemaphoreType.DMA((cols_n + rows_n,)),
        ],
        compiler_params=pltpu.CompilerParams(vmem_limit_bytes=40 * MIB),
    )(codes, counts, p_own, s_own, p_all, s_all)


def match_lists(p_codes, s_codes, q_ids, q_live, tile_cols, span):
    cols_n, p_max = p_codes.shape
    rows_n, s_max = s_codes.shape
    q_row, q_col = q_ids // tile_cols, q_ids % tile_cols
    at = jnp.arange(tile_cols, dtype=jnp.int32)
    p_want = q_row[:, None] * tile_cols + at[None, :]
    p_hit = p_codes[None, :, None, :] == p_want[:, None, :, None]
    p_slot = jnp.arange(cols_n * p_max, dtype=jnp.int32).reshape(1, cols_n, 1, p_max)
    p_at = jnp.max(jnp.where(p_hit, p_slot, -1), axis=3)
    level = jnp.arange(span * tile_cols, dtype=jnp.int32).reshape(span, tile_cols)
    s_want = level[None] * tile_cols + q_col[:, None, None]
    s_hit = s_codes[None, None, :, None, :] == s_want[:, :, None, :, None]
    s_slot = jnp.arange(rows_n * s_max, dtype=jnp.int32).reshape(1, 1, rows_n, 1, s_max)
    s_at = jnp.max(jnp.where(s_hit, s_slot, -1), axis=4)
    p_at = p_at.reshape(q_ids.shape[0], -1)
    s_at = s_at.reshape(q_ids.shape[0], -1)
    depth = p_at.shape[1]
    match = (p_at >= 0) & (s_at >= 0) & q_live[:, None]
    code = jnp.where(match, p_at * (rows_n * s_max) + s_at, 0)
    order = jnp.arange(depth, dtype=jnp.int32)
    before = order[None, :, None] > order[None, None, :]
    rank = jnp.sum((before & match[:, None, :]).astype(jnp.int32), axis=2)
    rank = jnp.where(match, rank, -1)
    picked = rank[:, None, :] == order[None, :, None]
    codes = jnp.sum(jnp.where(picked, code[:, None, :], 0), axis=2)
    return codes, jnp.sum(match.astype(jnp.int32), axis=1)


def on_device(coeffs, p_slots, p_count, s_blocks, s_slots, s_count, q_slots, q_count):
    rows_n = lax.axis_size("row")
    cols_n = lax.axis_size("col")
    tile_cols = coeffs.shape[0] * rows_n // cols_n // 128
    p_ids, s_ids, q_ids = p_slots[0, 0], s_slots[0, 0], q_slots[0, 0]
    s_own = s_blocks[0, 0]
    p_max, s_max, q_max = p_ids.shape[0], s_ids.shape[0], q_ids.shape[0]

    def live(ids, count):
        return jnp.arange(ids.shape[0], dtype=jnp.int32) < count[0, 0]

    def whole(p_codes, s_codes, p_own):
        codes, counts = match_lists(
            p_codes, s_codes, q_ids, live(q_ids, q_count), tile_cols, cols_n // rows_n
        )
        p_all, s_all = gather_blocks(p_own, s_own, rows_n, cols_n)
        return block_product(codes, counts, p_own, s_own, p_all, s_all)

    fits = tile_cols * cols_n == LANES and sum(one[0] for one in PHASES) == tile_cols
    if rows_n == 4 and fits and p_max == s_max == q_max == LANES // 2:
        counts = (p_count[0], q_count[0], s_count[0])
        p_own, p_pair, s_recv, codes, pairs, over, meta, *p_recv = panel_density(
            (p_ids, q_ids, s_ids), counts, coeffs, s_own, rows_n, cols_n
        )

        def full():
            row, col = lax.axis_index("row"), lax.axis_index("col")
            p_codes = lax.dynamic_index_in_dim(meta, row, 0, False)[:, 0, :p_max]
            s_codes = lax.dynamic_index_in_dim(meta, col, 1, False)[:, 2, :s_max]
            return whole(p_codes, s_codes, p_own)

        def packed():
            return packed_product(codes, pairs, [p_pair, *p_recv], [s_own, s_recv])

        product = lax.cond(jnp.max(over) > 0, full, packed)
    else:
        p_codes = lax.all_gather(jnp.where(live(p_ids, p_count), p_ids, -1), "col")
        s_codes = lax.all_gather(jnp.where(live(s_ids, s_count), s_ids, -1), "row")
        others = gather_rows(coeffs, rows_n, cols_n)
        p_own = density(p_ids, p_count[0], coeffs, others, rows_n, cols_n)
        product = whole(p_codes, s_codes, p_own)
    return (p_own.reshape(1, 1, p_max, 128, 128), product.reshape(1, 1, q_max, 128, 128))


def solution(mesh):
    return jax.shard_map(
        on_device,
        mesh=mesh,
        in_specs=(
            P("row", None),
            P("row", "col", None),
            P("row", "col"),
            P("row", "col", None, None, None),
            P("row", "col", None),
            P("row", "col"),
            P("row", "col", None),
            P("row", "col"),
        ),
        out_specs=(P("row", "col", None, None, None), P("row", "col", None, None, None)),
        check_vma=False,
    )
```

```python
import functools

import jax
import jax.numpy as jnp
from jax import lax
from jax.experimental import pallas as pl
from jax.experimental.pallas import tpu as pltpu
from jax.sharding import PartitionSpec as P

MESH = pl.DeviceIdType.MESH
MIB = 1 << 20
DEPTH = 3
BATCHES = (4, 8)
RING = 16
LANES = 128
CODE = 512
PHASES = ((10, 4, 5, 28), (6, 4, 3, 18))
LAG = 2
S_CAP = 42


def rows_kernel(rows_n, cols_n, coeffs, out, send, recv):
    row, col = lax.axis_index("row"), lax.axis_index("col")
    sub = cols_n // rows_n
    height = out.shape[0]
    piece = height // rows_n
    half, share = lax.rem(col, sub), lax.div(col, sub)
    owner = lax.div(col, sub)
    targets = [
        {"row": lax.rem(row + step, rows_n), "col": row * sub + half} for step in range(1, rows_n)
    ]
    sources = [{"row": owner, "col": part * sub + half} for part in range(rows_n)]
    barrier = pltpu.get_barrier_semaphore()
    for device in targets:
        pl.semaphore_signal(barrier, inc=1, device_id=device, device_id_type=MESH)

    @pl.when(row != owner)
    def _():
        for device in sources:
            pl.semaphore_signal(barrier, inc=1, device_id=device, device_id_type=MESH)

    pl.semaphore_wait(barrier, rows_n - 1 + jnp.where(row != owner, rows_n, 0))

    def copy(step, part, device):
        start = half * height + share * piece
        return pltpu.make_async_remote_copy(
            src_ref=coeffs.at[pl.ds(pl.multiple_of(start, piece), piece)],
            dst_ref=out.at[pl.ds(pl.multiple_of(part * piece, piece), piece)],
            send_sem=send.at[step],
            recv_sem=recv.at[part],
            device_id=device,
            device_id_type=MESH,
        )

    sends = [copy(step, share, device) for step, device in enumerate(targets)]
    for one in sends:
        one.start()

    @pl.when(row != owner)
    def _():
        for part, device in enumerate(sources):
            copy(0, part, device).wait_recv()

    for one in sends:
        one.wait_send()


def gather_rows(coeffs, rows_n, cols_n):
    height = coeffs.shape[0] * rows_n // cols_n
    body = functools.partial(rows_kernel, rows_n, cols_n)
    sems = [pltpu.SemaphoreType.DMA((rows_n - 1,)), pltpu.SemaphoreType.DMA((rows_n,))]
    return pl.pallas_call(
        body,
        out_shape=jax.ShapeDtypeStruct((height, coeffs.shape[1]), coeffs.dtype),
        in_specs=[pl.BlockSpec(memory_space=pl.ANY)],
        out_specs=pl.BlockSpec(memory_space=pl.ANY),
        scratch_shapes=sems,
        compiler_params=pltpu.CompilerParams(collective_id=0, has_side_effects=True),
    )(coeffs)


def density_kernel(rows_n, cols_n, ids, count, coeffs, others, out, left, right, sem):
    row, col = lax.axis_index("row"), lax.axis_index("col")
    sub = cols_n // rows_n
    height = others.shape[0]
    tile_cols = height // 128
    load_left = pltpu.make_async_copy(coeffs, left, sem.at[0])
    load_left.start()
    here = row == lax.div(col, sub)
    start = pl.multiple_of(lax.rem(col, sub) * height, height)
    load_own = pltpu.make_async_copy(coeffs.at[pl.ds(start, height)], right, sem.at[1])
    load_other = pltpu.make_async_copy(others, right, sem.at[1])

    @pl.when(here)
    def _():
        load_own.start()

    @pl.when(jnp.logical_not(here))
    def _():
        load_other.start()

    live = count[0]
    load_left.wait()
    load_other.wait()

    def block(slot, carry):
        a = pl.multiple_of(lax.div(ids[slot], tile_cols) * 128, 128)
        b = pl.multiple_of(lax.rem(ids[slot], tile_cols) * 128, 128)
        raw = lax.dot_general(
            left[pl.ds(a, 128), :],
            right[pl.ds(b, 128), :],
            (((1,), (1,)), ((), ())),
            preferred_element_type=jnp.float32,
        )
        out[slot] = raw.astype(out.dtype)
        return carry

    def clear(slot, carry):
        out[slot] = jnp.zeros(out.shape[1:], out.dtype)
        return carry

    lax.fori_loop(0, live, block, 0)
    lax.fori_loop(live, out.shape[0], clear, 0)


def density(ids, count, coeffs, others, rows_n, cols_n):
    slots = ids.shape[0]
    return pl.pallas_call(
        functools.partial(density_kernel, rows_n, cols_n),
        out_shape=jax.ShapeDtypeStruct((slots, 128, 128), jnp.bfloat16),
        in_specs=[pl.BlockSpec(memory_space=pltpu.SMEM)] * 2
        + [pl.BlockSpec(memory_space=pl.ANY)] * 2,
        out_specs=pl.BlockSpec(memory_space=pltpu.VMEM),
        scratch_shapes=[
            pltpu.VMEM(coeffs.shape, coeffs.dtype),
            pltpu.VMEM(others.shape, coeffs.dtype),
            pltpu.SemaphoreType.DMA((2,)),
        ],
        compiler_params=pltpu.CompilerParams(vmem_limit_bytes=40 * MIB),
    )(ids, count, coeffs, others)


def nt(x, y, precision=None):
    return lax.dot_general(
        x, y, (((1,), (1,)), ((), ())), precision=precision, preferred_element_type=jnp.float32
    )


def nn(x, y, precision=None):
    return jnp.dot(x, y, precision=precision, preferred_element_type=jnp.float32)


def iota(shape, dim):
    return lax.broadcasted_iota(jnp.int32, shape, dim)


def onehot(codes, height, kind=jnp.bfloat16):
    hit = iota((height, LANES), 0) == codes
    return jnp.where(hit, 1.0, 0.0).astype(kind)


def flat(x):
    return jnp.minimum(x, 1.0).astype(jnp.bfloat16)


def panel_kernel(rows_n, cols_n, phases, depth, *refs):
    stages = len(phases)
    ids, count, p_row, p_live, q_row, q_live, s_row, s_live, coeffs, s_in = refs[:10]
    p_pair_out, s_recv, codes, counts, flags_out, meta_out = refs[10:16]
    p_recv = refs[16 : 16 + stages]
    refs = refs[16 + stages :]
    right = []
    for _, chunks, _, _ in phases:
        right.append(refs[:chunks])
        refs = refs[chunks:]
    p_pair, p_pack = refs[:stages], refs[stages : 2 * stages]
    (
        left, total, s_pair, s_pack, meta, flags,
        p_dense, q_dense, q_wide, s_dense, p_need, p_rank, s_need, s_rank, lists, lists_s,
        send, recv, sem, meta_send, meta_recv, flag_send, flag_recv,
        pair_send, pair_recv, p_send, p_got, pass_send, pass_recv,
        s_send, s_got, s_pass_send, s_pass_recv, s_swap, done,
    ) = refs[2 * stages :]
    row, col = lax.axis_index("row"), lax.axis_index("col")
    slots = ids.shape[0]
    sub = cols_n // rows_n
    zs = cols_n // 2
    tile_rows = left.shape[0]
    tile_cols = sum(phase[0] for phase in phases)
    bits = tile_cols.bit_length() - 1
    caps = [phase[3] for phase in phases]
    starts = [sum(phase[0] for phase in phases[:f]) for f in range(stages)]
    bases = [2 * slots + zs * sum(caps[:f]) for f in range(stages)]
    s_cap = s_recv.shape[1] * s_recv.shape[2]
    z, core = lax.div(col, 2), lax.rem(col, 2)
    owner = lax.div(col, sub)
    first = lax.rem(col, sub) * tile_cols
    y, x = lax.div(row, 2), lax.rem(row, 2)
    dy = lax.rem(y + lax.div(owner, 2), 2)
    dx = lax.rem(x + lax.rem(owner, 2), 2)
    along_x, along_y = y * 2 + 1 - x, (1 - y) * 2 + x
    is_source = row == owner
    sends = [jnp.logical_or(dx == 1, dy == 0), jnp.logical_or(dx == 0, dy == 1)]
    following = [
        jnp.where(dx == dy, along_x, along_y),
        jnp.where(dx == dy, along_y, along_x),
    ]
    pieces = [(f, k) for f in range(stages) for k in range(phases[f][1])]
    steps = [(f, k, part) for f, k in pieces for part in range(phases[f][2])]
    partner = {"row": row, "col": z * 2 + 1 - core}
    row_mates = [{"row": row, "col": lax.rem(col + n, cols_n)} for n in range(1, cols_n)]
    col_mates = [{"row": lax.rem(row + n, rows_n), "col": col} for n in range(1, rows_n)]

    def remote(src, dst, send_sem, recv_sem, device):
        return pltpu.make_async_remote_copy(
            src_ref=src,
            dst_ref=dst,
            send_sem=send_sem,
            recv_sem=recv_sem,
            device_id=device,
            device_id_type=MESH,
        )

    def area(way, f, part):
        size = phases[f][0] // (2 * phases[f][2])
        return (way * phases[f][2] + part) * size, size

    def load(way, f, k, part):
        at, size = area(way, f, part)
        wide = right[f][k].shape[2]
        return pltpu.make_async_copy(
            coeffs.at[pl.ds(first + starts[f] + at, size), :, pl.ds(k * wide, wide)],
            right[f][k].at[pl.ds(at, size)],
            recv.at[way, steps.index((f, k, part))],
        )

    def copy(way, f, k, part):
        where = right[f][k].at[pl.ds(*area(way, f, part))]
        device = {"row": following[way], "col": col}
        at = steps.index((f, k, part))
        return remote(where, where, send.at[way, at], recv.at[way, at], device)

    @pl.when(is_source)
    def _():
        for step in steps:
            for way in range(2):
                load(way, *step).start()

    load_left = pltpu.make_async_copy(coeffs, left, sem.at[0])
    load_s = pltpu.make_async_copy(s_in, s_pair.at[pl.ds(core * slots, slots)], sem.at[1])
    load_left.start()
    load_s.start()

    mine = jnp.full((8, LANES), -1, jnp.int32)
    lane = iota((8, LANES), 1)
    height = iota((8, LANES), 0)
    for at, (codes_in, live_in) in enumerate(((p_row, p_live), (q_row, q_live), (s_row, s_live))):
        keep = jnp.logical_and(height == at, lane < live_in[0])
        mine = jnp.where(keep, codes_in[...], mine)
    meta[row, col] = mine

    barrier = pltpu.get_barrier_semaphore()
    for device in row_mates + col_mates:
        pl.semaphore_signal(barrier, inc=1, device_id=device, device_id_type=MESH)
    pl.semaphore_wait(barrier, len(row_mates) + len(col_mates))

    def along_row(table, send_sem, recv_sem, source, n):
        where = table.at[row, source]
        return remote(where, where, send_sem.at[n], recv_sem.at[source], row_mates[n])

    def along_col(table, send_sem, recv_sem, source, n):
        where = table.at[source]
        at = len(row_mates) + n
        return remote(where, where, send_sem.at[at], recv_sem.at[cols_n + source], col_mates[n])

    def spread(table, send_sem, recv_sem):
        def first_half():
            for n in range(cols_n - 1):
                along_row(table, send_sem, recv_sem, col, n).start()

        def second_half():
            for n in range(cols_n - 1):
                source = lax.rem(col + cols_n - 1 - n, cols_n)
                along_row(table, send_sem, recv_sem, source, n).wait_recv()
            for n in range(rows_n - 1):
                along_col(table, send_sem, recv_sem, row, n).start()

        def last():
            for n in range(rows_n - 1):
                source = lax.rem(row + rows_n - 1 - n, rows_n)
                along_col(table, send_sem, recv_sem, source, n).wait_recv()
            for n in range(cols_n - 1):
                along_row(table, send_sem, recv_sem, col, n).wait_send()
            for n in range(rows_n - 1):
                along_col(table, send_sem, recv_sem, row, n).wait_send()

        return first_half, second_half, last

    meta_steps = spread(meta, meta_send, meta_recv)
    flag_steps = spread(flags, flag_send, flag_recv)
    meta_steps[0]()

    def code(at, r, c):
        return meta[r, c][at : at + 1]

    def split(at, r, c):
        value = code(at, r, c)
        return value >> bits, c * tile_cols + (value & (tile_cols - 1))

    def split_s(r, c):
        value = code(2, r, c)
        local = value >> bits
        k = (r + rows_n * (local >> bits)) * tile_cols + (local & (tile_cols - 1))
        return k, c * tile_cols + (value & (tile_cols - 1))

    lanes = iota((1, LANES), 1)
    ahead = jnp.where(iota((LANES, LANES), 0) <= iota((LANES, LANES), 1), 1.0, 0.0)
    ahead = ahead.astype(jnp.bfloat16)
    exact = lax.Precision.HIGHEST

    def dense_rows(r):
        p_sum = jnp.zeros((LANES, tile_rows), jnp.float32)
        q_sum = jnp.zeros((LANES, tile_rows), jnp.float32)
        q_turn = jnp.zeros((tile_rows, LANES), jnp.float32)
        for c in range(cols_n):
            a, k = split(0, r, c)
            p_sum += nt(onehot(k, LANES), onehot(a, tile_rows))
            a, k = split(1, r, c)
            at_row, at_col = onehot(a, tile_rows), onehot(k, LANES)
            q_sum += nt(at_col, at_row)
            q_turn += nt(at_row, at_col)
        p_dense[r] = p_sum.astype(jnp.bfloat16)
        q_dense[r] = q_sum.astype(jnp.bfloat16)
        q_wide[r] = q_turn.astype(jnp.bfloat16)

    def dense_s():
        s_sum = jnp.zeros((LANES, LANES), jnp.float32)
        for r in range(rows_n):
            for c in range(cols_n):
                k, j = split_s(r, c)
                s_sum += nt(onehot(k, LANES), onehot(j, LANES))
        s_dense[...] = s_sum.astype(jnp.bfloat16)

    def ranked(need, rank, size):
        plain = nn(need[:size].astype(jnp.bfloat16), ahead)
        before = pltpu.roll(jnp.max(plain, axis=1, keepdims=True) + jnp.zeros_like(plain), 1, 0)
        odd = iota(plain.shape, 0) % 2 == 1
        rank[:size] = plain + jnp.where(odd, before, 0.0)

    def p_at(f, d, c):
        return (f * zs + d) * cols_n + c

    def s_at(r, source, half):
        return (r * rows_n + source) * 2 + half

    def need_p():
        wants = []
        for d in range(zs):
            group = lax.broadcasted_iota(jnp.int32, (tile_rows, LANES), 1) // (2 * tile_cols)
            part = jnp.where(group == d, q_wide[row].astype(jnp.float32), 0.0)
            wants.append(flat(nt(s_dense[...], part.astype(jnp.bfloat16))))
        for c in range(cols_n):
            a, k = split(0, row, c)
            at_row, at_k = onehot(a, tile_rows), onehot(k, LANES, jnp.float32)
            b = k - c * tile_cols
            for d in range(zs):
                hit = jnp.sum(nn(wants[d], at_row) * at_k, axis=0, keepdims=True)
                hit = jnp.minimum(hit, 1.0)
                for f in range(stages):
                    inside = jnp.logical_and(b >= starts[f], b < starts[f] + phases[f][0])
                    p_need[pl.ds(p_at(f, d, c), 1)] = jnp.where(inside, hit, 0.0)
        ranked(p_need, p_rank, stages * zs * cols_n)

    def need_s():
        for r in range(rows_n):
            wants = flat(nt(q_dense[r], p_dense[r]))
            for source in range(rows_n):
                for half in range(2):
                    k, j = split_s(source, z * 2 + half)
                    hit = nn(wants, onehot(k, LANES)) * onehot(j, LANES, jnp.float32)
                    hit = jnp.sum(hit, axis=0, keepdims=True)
                    s_need[pl.ds(s_at(r, source, half), 1)] = jnp.minimum(hit, 1.0)
        ranked(s_need, s_rank, rows_n * rows_n * 2)

    def picks(need, rank, base):
        chosen = jnp.logical_and(rank == (iota((LANES, LANES), 0) + 1).astype(jnp.float32), need > 0)
        chosen = jnp.where(chosen, 1.0, 0.0).astype(jnp.bfloat16)
        values = (base + lane).astype(jnp.float32).astype(jnp.bfloat16)
        return nt(values, chosen)

    def picked(need, rank, at):
        entry = jnp.zeros((8, LANES), jnp.float32)
        for half in range(2):
            row_at = pl.ds(at + half, 1)
            entry += picks(need[row_at], rank[row_at], half * slots)
        return entry

    def make_lists():
        for n in range(lists.shape[0] // 8):
            made = jnp.zeros((8, LANES), jnp.float32)
            for at in range(8):
                f, d = divmod(n * 8 + at, zs)
                r = n * 8 + at - stages * zs
                if f < stages:
                    entry = picked(p_need, p_rank, p_at(f, d, z * 2))
                elif r < rows_n:
                    entry = picked(s_need, s_rank, s_at(r, row, 0))
                else:
                    continue
                made = jnp.where(height == at, entry, made)
            lists[n * 8 : n * 8 + 8] = made.astype(jnp.int32)
        load_lists.start()

    def make_flags():
        over = jnp.zeros((1, 1), jnp.float32)
        for d in range(zs):
            for f in range(stages):
                most = jnp.max(p_rank[pl.ds(p_at(f, z, d * 2 + 1), 1)], axis=1, keepdims=True)
                over = jnp.maximum(over, jnp.where(d == z, 0.0, most - caps[f]))
        for r in range(rows_n):
            most = jnp.max(s_rank[pl.ds(s_at(row, r, 1), 1)], axis=1, keepdims=True)
            over = jnp.maximum(over, jnp.where(r == row, 0.0, most - s_cap))
        flags[row, col] = (over + jnp.zeros((8, LANES), jnp.float32)).astype(jnp.int32)
        flag_steps[0]()

    def make_codes():
        p_sum = jnp.zeros((tile_rows, LANES), jnp.float32)
        for c in range(cols_n):
            a, k = split(0, row, c)
            place = (c % 2 * slots + 1 + lanes).astype(jnp.float32)
            far = jnp.zeros((1, LANES), jnp.float32)
            for f in range(stages):
                at = pl.ds(p_at(f, z, c), 1)
                spot = bases[f] + c // 2 * caps[f] + p_rank[at]
                far = far + jnp.where(p_need[at] > 0, spot, 0.0)
            place = jnp.where(c // 2 == z, place, far)
            p_sum += nt(
                onehot(a, tile_rows, jnp.float32) * place, onehot(k, LANES, jnp.float32), exact
            )
        s_sum = jnp.zeros((LANES, LANES), jnp.float32)
        for r in range(rows_n):
            k, j = split_s(r, col)
            at = pl.ds(s_at(row, r, core), 1)
            far = jnp.where(s_need[at] > 0, slots + r * s_cap + s_rank[at], 0.0)
            place = jnp.where(r == row, (1 + lanes).astype(jnp.float32), far)
            s_sum += nt(onehot(j, LANES, jnp.float32) * place, onehot(k, LANES, jnp.float32), exact)
        a, j = split(1, row, col)
        unit = onehot(lanes, LANES)
        q_row_hot = nt(unit, onehot(a, tile_rows))[:slots]
        q_col_hot = nt(unit, onehot(j, LANES))[:slots]
        p_for = nn(q_row_hot, p_sum, exact)
        s_for = nn(q_col_hot, s_sum, exact)
        match = jnp.where(jnp.logical_and(p_for > 0, s_for > 0), 1.0, 0.0)
        value = (p_for - 1) * CODE + (s_for - 1)
        rank = nn(match.astype(jnp.bfloat16), ahead) * match
        counts[...] = nt(
            jnp.ones((8, LANES), jnp.bfloat16), match.astype(jnp.bfloat16)
        ).astype(jnp.int32)

        def place_one(n, made):
            here = jnp.where(rank == (n + 1).astype(jnp.float32), value, 0.0)
            here = jnp.sum(here, axis=1, keepdims=True)
            return jnp.where(iota(made.shape, 1) == n, here, made)

        made = jnp.zeros((slots, LANES), jnp.float32)
        made = lax.fori_loop(0, LANES, place_one, made, unroll=8)
        codes[...] = made.astype(jnp.int32)

    load_lists = pltpu.make_async_copy(lists, lists_s, sem.at[2])

    groups = 4
    group = slots // groups

    def pair_copy(f, n, half):
        where = p_pair[f].at[pl.ds(half * slots + n * group, group)]
        return remote(where, where, pair_send.at[f, n], pair_recv.at[f, n], partner)

    def s_pair_copy(half):
        where = s_pair.at[pl.ds(half * slots, slots)]
        return remote(where, where, s_swap.at[0], s_swap.at[1], partner)

    def chip(n):
        return lax.rem(z + n + 1, zs)

    def p_copy(f, n):
        device = {"row": row, "col": chip(n) * 2 + core}
        where = p_recv[f].at[z, core]
        return remote(p_pack[f].at[n], where, p_send.at[f, n], p_got.at[f, z], device)

    def p_arrival(f, n):
        where = p_recv[f].at[chip(n), core]
        return remote(p_pack[f].at[n], where, p_send.at[f, n], p_got.at[f, chip(n)], partner)

    def p_pass(f, n, half):
        where = p_recv[f].at[chip(n), half]
        return remote(where, where, pass_send.at[f, n], pass_recv.at[f, chip(n)], partner)

    def s_copy(n):
        where = s_recv.at[row, core]
        return remote(s_pack.at[n], where, s_send.at[n], s_got.at[row], col_mates[n])

    def s_arrival(n):
        source = col_mates[n]["row"]
        where = s_recv.at[source, core]
        return remote(s_pack.at[n], where, s_send.at[n], s_got.at[source], partner)

    def s_pass(n, half):
        source = col_mates[n]["row"]
        where = s_recv.at[source, half]
        return remote(where, where, s_pass_send.at[n], s_pass_recv.at[source], partner)

    def pack_p(f):
        for n in range(groups):
            pair_copy(f, n, 1 - core).wait_recv()
        half = caps[f] // 2
        for n in range(zs - 1):

            def fill(t, carry, n=n):
                at = lists_s[f * zs + chip(n), core * half + t]
                p_pack[f][n, t] = p_pair[f][jnp.clip(at, 0, 2 * slots - 1)]
                return carry

            lax.fori_loop(0, half, fill, 0)
            if f == stages - 1 or n == 0:
                p_copy(f, n).start()

    def pack_s():
        s_pair_copy(1 - core).wait_recv()
        half = s_cap // 2
        for n in range(rows_n - 1):

            def fill(t, carry, n=n):
                at = lists_s[stages * zs + col_mates[n]["row"], core * half + t]
                s_pack[n, t] = s_pair[jnp.clip(at, 0, 2 * slots - 1)]
                return carry

            lax.fori_loop(0, half, fill, 0)

    def start_swap():
        load_s.wait()
        s_pair_copy(core).start()

    ready = phases[0][1]
    idle = [lambda: None]
    ready = phases[0][1]
    work = {
        0: [meta_steps[1]] + idle * 3 + [start_swap],
        1: [meta_steps[2]] + [functools.partial(dense_rows, r) for r in range(rows_n)],
        2: [dense_s, idle[0], need_p],
        3: [need_s, idle[0], make_lists],
        ready: [load_lists.wait, lambda: pack_p(0), make_flags],
        ready + 1: [p_copy(0, 1).start, flag_steps[1], make_codes],
        ready + 2: [flag_steps[2], idle[0], pack_s],
        ready + 3: [p_copy(0, 2).start],
    }

    def relay(n, part):
        f, k = pieces[n]
        now = steps.index((f, k, part))
        for way in range(2):

            @pl.when(sends[way])
            def _():
                copy(way, f, k, part).wait_recv()
                if now >= depth:
                    copy(way, *steps[now - depth]).wait_send()
                copy(way, f, k, part).start()

    for n in range(LAG):
        for part in range(phases[pieces[n][0]][2]):
            relay(n, part)
    load_left.wait()
    for n, (f, k) in enumerate(pieces):
        for way in range(2):

            @pl.when(jnp.logical_not(sends[way]))
            def _():
                for part in range(phases[f][2]):
                    copy(way, f, k, part).wait_recv()

        if n == len(pieces) - 1:
            for one in range(rows_n - 1):
                s_copy(one).start()
        wide = right[f][k].shape[2]
        ends = k == phases[f][1] - 1

        def blocks(step, carry, f=f, k=k, wide=wide, ends=ends, batch=BATCHES[f]):
            slot = [step * batch + one for one in range(batch)]
            b = [(ids[at] & (tile_cols - 1)) - starts[f] for at in slot]
            raw = [
                lax.dot_general(
                    left[ids[at] >> bits, :, pl.ds(k * wide, wide)],
                    right[f][k][jnp.clip(where, 0, phases[f][0] - 1)],
                    (((1,), (1,)), ((), ())),
                    preferred_element_type=jnp.float32,
                )
                for at, where in zip(slot, b)
            ]
            if k > 0:
                raw = [one + total[at] for one, at in zip(raw, slot)]
            if not ends:
                for one, at in zip(raw, slot):
                    total[at] = one
                return carry
            made = []
            for one, at, where in zip(raw, slot, b):
                inside = jnp.logical_and(where >= 0, where < phases[f][0])
                inside = jnp.logical_and(inside, at < count[0])
                other = 0.0
                if f > 0:
                    other = p_pair[f - 1][core * slots + at].astype(jnp.float32)
                made.append(jnp.where(inside, one, other).astype(p_pair[f].dtype))
            for one, at in zip(made, slot):
                p_pair[f][core * slots + at] = one
            return carry

        todo = list(work.get(n, []))
        later = n + LAG
        if later < len(pieces):
            pulls = [functools.partial(relay, later, p) for p in range(phases[pieces[later][0]][2])]
        else:
            pulls = []
        turns = groups if ends else max(len(pulls), len(todo), 1)
        batches = slots // BATCHES[f]
        for turn in range(turns):
            if turn < len(pulls):
                pulls[turn]()
            low, high = batches * turn // turns, batches * (turn + 1) // turns
            lax.fori_loop(low, high, blocks, 0)
            if ends:
                pair_copy(f, turn, core).start()
            if turn < len(todo):
                todo[turn]()
        for one in pulls[turns:] + todo[turns:]:
            one()

    final = p_pair[-1]
    pack_p(stages - 1)
    pair_out = pltpu.make_async_copy(final, p_pair_out, done.at[1])
    flags_go = pltpu.make_async_copy(flags, flags_out, done.at[2])
    meta_go = pltpu.make_async_copy(meta, meta_out, done.at[3])
    for one in (pair_out, flags_go, meta_go):
        one.start()
    for way in range(2):

        @pl.when(sends[way])
        def _():
            for step in steps[-depth:]:
                copy(way, *step).wait_send()

    s_pair_copy(core).wait_send()
    for f in range(stages):
        for n in range(groups):
            pair_copy(f, n, core).wait_send()
    for f in range(stages):
        if f == stages - 1:
            for n in range(rows_n - 1):
                s_arrival(n).wait_recv()
                s_pass(n, core).start()
        for n in range(zs - 1):
            p_arrival(f, n).wait_recv()
            p_pass(f, n, core).start()
    for n in range(rows_n - 1):
        s_pass(n, 1 - core).wait_recv()
        s_pass(n, core).wait_send()
        s_copy(n).wait_send()
    for f in range(stages):
        for n in range(zs - 1):
            p_pass(f, n, 1 - core).wait_recv()
            p_pass(f, n, core).wait_send()
            p_copy(f, n).wait_send()
    for one in (pair_out, flags_go, meta_go):
        one.wait()


def panel_density(ids, counts, coeffs, s_own, rows_n, cols_n):
    slots = ids[0].shape[0]
    orbitals = coeffs.shape[1]
    blocks = coeffs.reshape(-1, 128, orbitals)
    tile_rows = blocks.shape[0]
    zs = cols_n // 2
    stages = len(PHASES)
    kind = coeffs.dtype
    block = (128, 128)
    smem, vmem = pl.BlockSpec(memory_space=pltpu.SMEM), pl.BlockSpec(memory_space=pltpu.VMEM)
    anywhere = pl.BlockSpec(memory_space=pl.ANY)
    rows = [jnp.pad(one[None], ((0, 0), (0, LANES - slots)), constant_values=-1) for one in ids]
    table = (rows_n, cols_n, 8, LANES)
    sems = pltpu.SemaphoreType.DMA
    steps = sum(chunks * parts for _, chunks, parts, _ in PHASES)
    p_rows, s_rows = stages * zs * cols_n + 8, rows_n * rows_n * 2 + 8
    list_rows = -(-(stages * zs + rows_n) // 8) * 8
    mates = cols_n + rows_n - 2
    panels = [
        pltpu.VMEM((wide, 128, orbitals // chunks), kind)
        for wide, chunks, _, _ in PHASES
        for _ in range(chunks)
    ]
    return pl.pallas_call(
        functools.partial(panel_kernel, rows_n, cols_n, PHASES, DEPTH),
        out_shape=[
            jax.ShapeDtypeStruct((2 * slots,) + block, kind),
            jax.ShapeDtypeStruct((rows_n, 2, S_CAP // 2) + block, kind),
            jax.ShapeDtypeStruct((slots, LANES), jnp.int32),
            jax.ShapeDtypeStruct((8, slots), jnp.int32),
            jax.ShapeDtypeStruct(table, jnp.int32),
            jax.ShapeDtypeStruct(table, jnp.int32),
        ]
        + [jax.ShapeDtypeStruct((zs, 2, cap // 2) + block, kind) for _, _, _, cap in PHASES],
        in_specs=[smem, smem] + [vmem, smem] * 3 + [anywhere] * 2,
        out_specs=[anywhere] * 2 + [vmem] * 2 + [anywhere] * (2 + stages),
        scratch_shapes=panels
        + [pltpu.VMEM((2 * slots,) + block, kind)] * stages
        + [pltpu.VMEM((zs - 1, cap // 2) + block, kind) for _, _, _, cap in PHASES]
        + [
            pltpu.VMEM(blocks.shape, kind),
            pltpu.VMEM((slots,) + block, jnp.float32),
            pltpu.VMEM((2 * slots,) + block, kind),
            pltpu.VMEM((rows_n - 1, S_CAP // 2) + block, kind),
            pltpu.VMEM(table, jnp.int32),
            pltpu.VMEM(table, jnp.int32),
            pltpu.VMEM((rows_n, LANES, tile_rows), jnp.bfloat16),
            pltpu.VMEM((rows_n, LANES, tile_rows), jnp.bfloat16),
            pltpu.VMEM((rows_n, tile_rows, LANES), jnp.bfloat16),
            pltpu.VMEM((LANES, LANES), jnp.bfloat16),
            pltpu.VMEM((p_rows, LANES), jnp.float32),
            pltpu.VMEM((p_rows, LANES), jnp.float32),
            pltpu.VMEM((s_rows, LANES), jnp.float32),
            pltpu.VMEM((s_rows, LANES), jnp.float32),
            pltpu.VMEM((list_rows, LANES), jnp.int32),
            pltpu.SMEM((list_rows, LANES), jnp.int32),
            sems((2, steps)),
            sems((2, steps)),
            sems((3,)),
            sems((mates,)),
            sems((cols_n + rows_n,)),
            sems((mates,)),
            sems((cols_n + rows_n,)),
            sems((stages, 4)),
            sems((stages, 4)),
            sems((stages, zs - 1)),
            sems((stages, zs)),
            sems((stages, zs - 1)),
            sems((stages, zs)),
            sems((rows_n - 1,)),
            sems((rows_n,)),
            sems((rows_n - 1,)),
            sems((rows_n,)),
            sems((2,)),
            sems((4,)),
        ],
        compiler_params=pltpu.CompilerParams(
            collective_id=2, has_side_effects=True, vmem_limit_bytes=60 * MIB
        ),
    )(ids[0], counts[0], rows[0], counts[0], rows[1], counts[1], rows[2], counts[2], blocks, s_own)


def packed_kernel(p_many, slots, codes, counts, *refs):
    p_parts, s_parts = refs[:p_many], refs[p_many:-8]
    out, density, left, right, own, flat, sem, done = refs[-8:]
    core = lax.rem(lax.axis_index("col"), 2)
    own_in = pltpu.make_async_copy(p_parts[0].at[pl.ds(core * slots, slots)], own, done.at[0])
    own_out = pltpu.make_async_copy(own, density, done.at[1])
    own_in.start()

    def listed(q, at):
        def one(n, at):
            flat[at] = codes[q, n]
            return at + 1

        return lax.fori_loop(0, counts[0, q], one, at)

    pairs = lax.fori_loop(0, slots, listed, 0)

    def fetch(at):
        spot = lax.rem(at, RING)
        code = flat[at]
        for side, (where, parts, ring) in enumerate(
            ((lax.div(code, CODE), p_parts, left), (lax.rem(code, CODE), s_parts, right))
        ):
            low = 0
            for part in parts:
                high = low + part.shape[0]

                @pl.when(jnp.logical_and(where >= low, where < high))
                def _():
                    pltpu.make_async_copy(
                        part.at[where - low], ring.at[spot], sem.at[side, spot]
                    ).start()

                low = high

    def ahead(at, carry):
        fetch(at)
        return carry

    lax.fori_loop(0, jnp.minimum(pairs, RING), ahead, 0)
    own_in.wait()
    own_out.start()

    def slot(q, at):
        def term(n, total):
            now = at + n
            spot = lax.rem(now, RING)
            pltpu.make_async_copy(p_parts[0].at[0], left.at[spot], sem.at[0, spot]).wait()
            pltpu.make_async_copy(s_parts[0].at[0], right.at[spot], sem.at[1, spot]).wait()
            total += jnp.dot(left[spot], right[spot], preferred_element_type=jnp.float32)

            @pl.when(now + RING < pairs)
            def _():
                fetch(now + RING)

            return total

        many = counts[0, q]
        out[q] = lax.fori_loop(0, many, term, jnp.zeros((128, 128), jnp.float32))
        return at + many

    lax.fori_loop(0, slots, slot, 0)
    own_out.wait()


def packed_product(codes, counts, p_parts, s_parts):
    p_parts = [part.reshape(-1, 128, 128) for part in p_parts]
    s_parts = [part.reshape(-1, 128, 128) for part in s_parts]
    kind = s_parts[0].dtype
    slots = codes.shape[0]
    many = len(p_parts) + len(s_parts)
    block = (128, 128)
    return pl.pallas_call(
        functools.partial(packed_kernel, len(p_parts), slots),
        out_shape=[
            jax.ShapeDtypeStruct((slots,) + block, jnp.float32),
            jax.ShapeDtypeStruct((slots,) + block, kind),
        ],
        in_specs=[pl.BlockSpec(memory_space=pltpu.SMEM)] * 2
        + [pl.BlockSpec(memory_space=pl.ANY)] * many,
        out_specs=[
            pl.BlockSpec(memory_space=pltpu.VMEM),
            pl.BlockSpec(memory_space=pl.ANY),
        ],
        scratch_shapes=[
            pltpu.VMEM((RING,) + block, kind),
            pltpu.VMEM((RING,) + block, kind),
            pltpu.VMEM((slots,) + block, kind),
            pltpu.SMEM((codes.size,), jnp.int32),
            pltpu.SemaphoreType.DMA((2, RING)),
            pltpu.SemaphoreType.DMA((2,)),
        ],
        compiler_params=pltpu.CompilerParams(vmem_limit_bytes=40 * MIB),
    )(codes, counts, *p_parts, *s_parts)


def blocks_kernel(rows_n, cols_n, parts, p_own, s_own, p_all, s_all, *sems):
    send, recv, pass_send, pass_recv, s_send, s_recv = sems
    row, col = lax.axis_index("row"), lax.axis_index("col")
    length = cols_n // 2
    z, core = lax.div(col, 2), lax.rem(col, 2)
    size = p_own.shape[0] // parts
    right, left = {"row": row, "col": col + 2}, {"row": row, "col": col - 2}
    partner = {"row": row, "col": z * 2 + 1 - core}
    column = [{"row": lax.rem(row + step, rows_n), "col": col} for step in range(1, rows_n)]
    has_right, has_left = z + 1 < length, z > 0

    barrier = pltpu.get_barrier_semaphore()

    def greet(device):
        pl.semaphore_signal(barrier, inc=1, device_id=device, device_id_type=MESH)

    greet(partner)
    for device in column:
        greet(device)

    @pl.when(has_right)
    def _():
        greet(right)

    @pl.when(has_left)
    def _():
        greet(left)

    pl.semaphore_wait(barrier, rows_n + jnp.where(has_right, 1, 0) + jnp.where(has_left, 1, 0))

    def remote(src, dst, send_sem, recv_sem, device):
        return pltpu.make_async_remote_copy(
            src_ref=src,
            dst_ref=dst,
            send_sem=send_sem,
            recv_sem=recv_sem,
            device_id=device,
            device_id_type=MESH,
        )

    def piece(source, lane, part):
        return p_all.at[source * 2 + lane, pl.ds(part * size, size)]

    def origin(way, step):
        return z - step if way == 0 else z + step

    def sent(way, step, part):
        where = piece(origin(way, step), core, part)
        src = p_own.at[pl.ds(part * size, size)] if step == 0 else where
        device = right if way == 0 else left
        return remote(src, where, send.at[way, step, part], recv.at[way, step, part], device)

    def passed(way, step, part):
        where = piece(origin(way, step), core, part)
        src = p_own.at[pl.ds(part * size, size)] if step == 0 else where
        return remote(
            src, where, pass_send.at[way, step, part], pass_recv.at[way, step, part], partner
        )

    def onward(way):
        return has_right if way == 0 else has_left

    def exists(way, step):
        return z >= step if way == 0 else z + step < length

    for part in range(parts):
        for way in range(2):
            pl.when(onward(way))(lambda way=way: sent(way, 0, part).start())
    s_sends = [
        remote(s_own, s_all.at[row], s_send.at[n], s_recv.at[n], device)
        for n, device in enumerate(column)
    ]
    for one in s_sends:
        one.start()
    for part in range(parts):
        passed(0, 0, part).start()
    for step in range(1, length):
        for part in range(parts):
            for way in range(2):

                @pl.when(exists(way, step))
                def _():
                    sent(way, step - 1, part).wait_recv()
                    passed(way, step, part).start()
                    if step < length - 1:
                        pl.when(onward(way))(lambda: sent(way, step, part).start())

    for part in range(parts):
        passed(0, 0, part).wait()
        for way in range(2):
            pl.when(onward(way))(lambda way=way: sent(way, 0, part).wait_send())
    for step in range(1, length):
        for part in range(parts):
            for way in range(2):

                @pl.when(exists(way, step))
                def _():
                    passed(way, step, part).wait()
                    if step < length - 1:
                        pl.when(onward(way))(lambda: sent(way, step, part).wait_send())

    for one in s_sends:
        one.wait()


def gather_blocks(p_own, s_own, rows_n, cols_n):
    parts = 4 if p_own.shape[0] % 4 == 0 else 1
    table = pltpu.SemaphoreType.DMA((2, cols_n // 2, parts))
    return pl.pallas_call(
        functools.partial(blocks_kernel, rows_n, cols_n, parts),
        out_shape=(
            jax.ShapeDtypeStruct((cols_n,) + p_own.shape, p_own.dtype),
            jax.ShapeDtypeStruct((rows_n,) + s_own.shape, s_own.dtype),
        ),
        in_specs=[pl.BlockSpec(memory_space=pl.ANY)] * 2,
        out_specs=[pl.BlockSpec(memory_space=pl.ANY)] * 2,
        scratch_shapes=[table] * 4 + [pltpu.SemaphoreType.DMA((rows_n - 1,))] * 2,
        compiler_params=pltpu.CompilerParams(collective_id=1, has_side_effects=True),
    )(p_own, s_own)


def product_kernel(rows_n, cols_n, codes, counts, p_own, s_own, p_all, s_all, out, left, right, sem):
    row, col = lax.axis_index("row"), lax.axis_index("col")
    p_max, s_max = p_own.shape[0], s_own.shape[0]
    base = rows_n * s_max
    loads = [pltpu.make_async_copy(p_own, left.at[pl.ds(col * p_max, p_max)], sem.at[0])]
    loads += [pltpu.make_async_copy(s_own, right.at[pl.ds(row * s_max, s_max)], sem.at[1])]
    for step in range(1, cols_n):
        at = lax.rem(col + step, cols_n)
        loads += [
            pltpu.make_async_copy(
                p_all.at[at], left.at[pl.ds(at * p_max, p_max)], sem.at[len(loads)]
            )
        ]
    for step in range(1, rows_n):
        at = lax.rem(row + step, rows_n)
        loads += [
            pltpu.make_async_copy(
                s_all.at[at], right.at[pl.ds(at * s_max, s_max)], sem.at[len(loads)]
            )
        ]
    for load in loads:
        load.start()
    for load in loads:
        load.wait()

    def slot(q, carry):
        def term(n, total):
            code = codes[q, n]
            return total + jnp.dot(
                left[lax.div(code, base)],
                right[lax.rem(code, base)],
                preferred_element_type=jnp.float32,
            )

        out[q] = lax.fori_loop(0, counts[q], term, jnp.zeros((128, 128), jnp.float32))
        return carry

    lax.fori_loop(0, out.shape[0], slot, 0)


def block_product(codes, counts, p_own, s_own, p_all, s_all):
    cols_n, p_max = p_all.shape[:2]
    rows_n, s_max = s_all.shape[:2]
    return pl.pallas_call(
        functools.partial(product_kernel, rows_n, cols_n),
        out_shape=jax.ShapeDtypeStruct((counts.shape[0], 128, 128), jnp.float32),
        in_specs=[pl.BlockSpec(memory_space=pltpu.SMEM)] * 2
        + [pl.BlockSpec(memory_space=pl.ANY)] * 4,
        out_specs=pl.BlockSpec(memory_space=pltpu.VMEM),
        scratch_shapes=[
            pltpu.VMEM((cols_n * p_max, 128, 128), p_all.dtype),
            pltpu.VMEM((rows_n * s_max, 128, 128), s_all.dtype),
            pltpu.SemaphoreType.DMA((cols_n + rows_n,)),
        ],
        compiler_params=pltpu.CompilerParams(vmem_limit_bytes=40 * MIB),
    )(codes, counts, p_own, s_own, p_all, s_all)


def match_lists(p_codes, s_codes, q_ids, q_live, tile_cols, span):
    cols_n, p_max = p_codes.shape
    rows_n, s_max = s_codes.shape
    q_row, q_col = q_ids // tile_cols, q_ids % tile_cols
    at = jnp.arange(tile_cols, dtype=jnp.int32)
    p_want = q_row[:, None] * tile_cols + at[None, :]
    p_hit = p_codes[None, :, None, :] == p_want[:, None, :, None]
    p_slot = jnp.arange(cols_n * p_max, dtype=jnp.int32).reshape(1, cols_n, 1, p_max)
    p_at = jnp.max(jnp.where(p_hit, p_slot, -1), axis=3)
    level = jnp.arange(span * tile_cols, dtype=jnp.int32).reshape(span, tile_cols)
    s_want = level[None] * tile_cols + q_col[:, None, None]
    s_hit = s_codes[None, None, :, None, :] == s_want[:, :, None, :, None]
    s_slot = jnp.arange(rows_n * s_max, dtype=jnp.int32).reshape(1, 1, rows_n, 1, s_max)
    s_at = jnp.max(jnp.where(s_hit, s_slot, -1), axis=4)
    p_at = p_at.reshape(q_ids.shape[0], -1)
    s_at = s_at.reshape(q_ids.shape[0], -1)
    depth = p_at.shape[1]
    match = (p_at >= 0) & (s_at >= 0) & q_live[:, None]
    code = jnp.where(match, p_at * (rows_n * s_max) + s_at, 0)
    order = jnp.arange(depth, dtype=jnp.int32)
    before = order[None, :, None] > order[None, None, :]
    rank = jnp.sum((before & match[:, None, :]).astype(jnp.int32), axis=2)
    rank = jnp.where(match, rank, -1)
    picked = rank[:, None, :] == order[None, :, None]
    codes = jnp.sum(jnp.where(picked, code[:, None, :], 0), axis=2)
    return codes, jnp.sum(match.astype(jnp.int32), axis=1)


def on_device(coeffs, p_slots, p_count, s_blocks, s_slots, s_count, q_slots, q_count):
    rows_n = lax.axis_size("row")
    cols_n = lax.axis_size("col")
    tile_cols = coeffs.shape[0] * rows_n // cols_n // 128
    p_ids, s_ids, q_ids = p_slots[0, 0], s_slots[0, 0], q_slots[0, 0]
    s_own = s_blocks[0, 0]
    p_max, s_max, q_max = p_ids.shape[0], s_ids.shape[0], q_ids.shape[0]

    def live(ids, count):
        return jnp.arange(ids.shape[0], dtype=jnp.int32) < count[0, 0]

    def whole(p_codes, s_codes, p_own):
        codes, counts = match_lists(
            p_codes, s_codes, q_ids, live(q_ids, q_count), tile_cols, cols_n // rows_n
        )
        p_all, s_all = gather_blocks(p_own, s_own, rows_n, cols_n)
        return block_product(codes, counts, p_own, s_own, p_all, s_all)

    fits = tile_cols * cols_n == LANES and sum(one[0] for one in PHASES) == tile_cols
    if rows_n == 4 and fits and p_max == s_max == q_max == LANES // 2:
        counts = (p_count[0], q_count[0], s_count[0])
        p_pair, s_recv, codes, pairs, over, meta, *p_recv = panel_density(
            (p_ids, q_ids, s_ids), counts, coeffs, s_own, rows_n, cols_n
        )

        def full():
            row, col = lax.axis_index("row"), lax.axis_index("col")
            p_codes = lax.dynamic_index_in_dim(meta, row, 0, False)[:, 0, :p_max]
            s_codes = lax.dynamic_index_in_dim(meta, col, 1, False)[:, 2, :s_max]
            p_own = lax.dynamic_slice_in_dim(p_pair, col % 2 * p_max, p_max)
            return whole(p_codes, s_codes, p_own), p_own

        def packed():
            return packed_product(codes, pairs, [p_pair, *p_recv], [s_own, s_recv])

        product, p_own = lax.cond(jnp.max(over) > 0, full, packed)
    else:
        p_codes = lax.all_gather(jnp.where(live(p_ids, p_count), p_ids, -1), "col")
        s_codes = lax.all_gather(jnp.where(live(s_ids, s_count), s_ids, -1), "row")
        others = gather_rows(coeffs, rows_n, cols_n)
        p_own = density(p_ids, p_count[0], coeffs, others, rows_n, cols_n)
        product = whole(p_codes, s_codes, p_own)
    return (p_own.reshape(1, 1, p_max, 128, 128), product.reshape(1, 1, q_max, 128, 128))


def solution(mesh):
    return jax.shard_map(
        on_device,
        mesh=mesh,
        in_specs=(
            P("row", None),
            P("row", "col", None),
            P("row", "col"),
            P("row", "col", None, None, None),
            P("row", "col", None),
            P("row", "col"),
            P("row", "col", None),
            P("row", "col"),
        ),
        out_specs=(P("row", "col", None, None, None), P("row", "col", None, None, None)),
        check_vma=False,
    )
```
